256 devices in a mesh: gx: 4 (over x), gy: 8 (over z_lo, y), gz: 8 (over z_hi, core).
Axes of the slice: x: 4, y: 4, z: 8 (z_hi: 4, z_lo: 2; z = z_hi * 2 + z_lo), core: 2. Of those that a mesh axis runs over, the one named last changes fastest.
Arguments:
- charges: float32 [128, 512, 1024], P('gx', 'gy', 'gz'), may hold values from -8 to 8
- kernel_taps: float32 [5, 3, 17], replicated, may hold values from 0.08 to 0.4
Outputs:
- potential: float32 [128, 512, 1024], P('gx', 'gy', 'gz')
The draws below stay inside these ranges and needn't reach their ends.
All inputs are finite; a program needn't handle non-finite values.
Results may differ from the reference program's by a relative error of at most 0.00029.
Values sent between devices are 32-bit elements; how exact they have to be, the bound alone decides.
No kernel may reach another device: no remote copies, remote signals or barrier semaphores. Data moves between devices by JAX's collectives and lax.ppermute only.
A program may use at most 128 MiB of HBM per device.

```python
import math
import jax
import jax.numpy as jnp
from jax import lax

LEVELS = 5
TAPS = 17
NX = 128
NY = 512
NZ = 1024


def block_levels(stream_key, shape, cuts, smallest, top_value):
    def one(dim, blocks):
        steps = jax.random.uniform(jax.random.fold_in(jax.random.fold_in(stream_key, 6), dim), (blocks,), jnp.float32, smallest / len(cuts), top_value / len(cuts))
        return jnp.repeat(jnp.exp(steps), shape[dim] // blocks).reshape((-1,) + (1,) * (len(shape) - dim - 1))

    loudness = one(*cuts[0])
    for cut in cuts[1:]:
        loudness = loudness * one(*cut)
    return loudness


def normal_values(stream_key, shape, width, most, shards=(), kind=jnp.bfloat16):
    factor_of = block_levels(stream_key, shape, shards, -0.22, 0.18) if shards else 1.0
    values = jax.random.normal(stream_key, shape, jnp.float32) * width * factor_of
    return jnp.minimum(jnp.maximum(values, -most), most).astype(kind)


def setup_inputs(seed: int = 0) -> dict:
    arg_keys = jax.random.split(jax.random.key(seed), 3)
    charges = normal_values(arg_keys[0], (NX, NY, NZ), 1.0, 8.0, ((0, 4), (1, 8), (2, 8)), jnp.float32)
    kernel_taps = jnp.clip(jnp.exp(jax.random.uniform(arg_keys[1], (LEVELS, 3, TAPS), jnp.float32, math.log(0.08), math.log(0.4))), 0.08, 0.4)
    return dict(charges=charges, kernel_taps=kernel_taps)


CUBIC = (-0.0625, 0.0, 0.5625, 1.0, 0.5625, 0.0, -0.0625)
PATTERNS = ("ij,jbc->ibc", "ij,ajc->aic", "ij,abj->abi")


def picks_matrix(weights, offsets):
    count = weights.shape[0]
    picks = (offsets[None, :, :] == jnp.arange(count, dtype=jnp.int32)[:, None, None]).astype(jnp.float32)
    return jnp.sum(weights.astype(jnp.float32)[:, None, None] * picks, axis=0)


def apply_axis(matrix, values, axis):
    return jnp.einsum(PATTERNS[axis], matrix, values, precision=lax.Precision.HIGHEST)


def stencil_padded(padded, taps_level):
    for axis in range(3):
        length = padded.shape[axis] - 16
        total = jnp.zeros(padded.shape[:axis] + (length,) + padded.shape[axis + 1:], jnp.float32)
        for offset in range(17):
            total = total + taps_level[axis, offset] * lax.slice_in_dim(padded, offset, offset + length, 1, axis)
        padded = total
    return padded


def restrict_padded(padded):
    cubic = jnp.array(CUBIC, jnp.float32)
    for axis in range(3):
        length = padded.shape[axis] - 6
        offsets = jnp.arange(length + 6, dtype=jnp.int32)[None, :] - 2 * jnp.arange(length // 2, dtype=jnp.int32)[:, None]
        padded = apply_axis(picks_matrix(cubic, offsets), padded, axis)
    return padded


def prolong_padded(padded):
    cubic = jnp.array(CUBIC, jnp.float32)
    for axis in range(3):
        length = padded.shape[axis] - 4
        offsets = 7 + jnp.arange(2 * length, dtype=jnp.int32)[:, None] - 2 * jnp.arange(length + 4, dtype=jnp.int32)[None, :]
        padded = apply_axis(picks_matrix(cubic, offsets), padded, axis)
    return padded


def reference(charges, kernel_taps):
    levels_charge = [charges]
    for level in range(1, LEVELS):
        levels_charge.append(restrict_padded(jnp.pad(levels_charge[-1], 3)))
    result = stencil_padded(jnp.pad(levels_charge[LEVELS - 1], 8), kernel_taps[LEVELS - 1])
    for level in range(LEVELS - 2, -1, -1):
        result = stencil_padded(jnp.pad(levels_charge[level], 8), kernel_taps[level]) + prolong_padded(jnp.pad(result, 2))
    return result
```

```python
import jax
import jax.numpy as jnp
from jax import lax
from jax.sharding import PartitionSpec as P

LEVELS = 5


CUBIC = (-0.0625, 0.0, 0.5625, 1.0, 0.5625, 0.0, -0.0625)
PATTERNS = ("ij,jbc->ibc", "ij,ajc->aic", "ij,abj->abi")


def extended(block, sides, width):
    for axis, dim in sides:
        count = lax.axis_size(axis)
        forward = [(i, i + 1) for i in range(count - 1)]
        backward = [(target, source) for source, target in forward]
        low = lax.ppermute(
            lax.slice_in_dim(block, block.shape[dim] - width, None, axis=dim), axis, forward
        )
        high = lax.ppermute(lax.slice_in_dim(block, 0, width, axis=dim), axis, backward)
        block = jnp.concatenate([low, block, high], axis=dim)
    return block


def picks_matrix(weights, offsets):
    count = weights.shape[0]
    picks = (offsets[None, :, :] == jnp.arange(count, dtype=jnp.int32)[:, None, None]).astype(
        jnp.float32
    )
    return jnp.sum(weights[:, None, None] * picks, axis=0)


def apply_axis(matrix, values, axis):
    return jnp.einsum(PATTERNS[axis], matrix, values, precision=lax.Precision.HIGHEST)


def stencil_axis(padded, taps_row, axis):
    length = padded.shape[axis] - 16
    offsets = (
        jnp.arange(length + 16, dtype=jnp.int32)[None, :]
        - jnp.arange(length, dtype=jnp.int32)[:, None]
    )
    return apply_axis(picks_matrix(taps_row, offsets), padded, axis)


def stencil_padded(padded, taps_level):
    for axis in range(3):
        padded = stencil_axis(padded, taps_level[axis], axis)
    return padded


def restrict_padded(padded):
    cubic = jnp.array(CUBIC, jnp.float32)
    for axis in range(3):
        length = padded.shape[axis] - 6
        offsets = (
            jnp.arange(length + 6, dtype=jnp.int32)[None, :]
            - 2 * jnp.arange(length // 2, dtype=jnp.int32)[:, None]
        )
        padded = apply_axis(picks_matrix(cubic, offsets), padded, axis)
    return padded


def prolong_padded(padded):
    cubic = jnp.array(CUBIC, jnp.float32)
    for axis in range(3):
        length = padded.shape[axis] - 4
        offsets = (
            7
            + jnp.arange(2 * length, dtype=jnp.int32)[:, None]
            - 2 * jnp.arange(length + 4, dtype=jnp.int32)[None, :]
        )
        padded = apply_axis(picks_matrix(cubic, offsets), padded, axis)
    return padded


def per_device(charges, kernel_taps):
    top_level = 3
    direct_terms = []
    grid_now = charges
    for level in range(top_level):
        padded = extended(grid_now, (("gx", 0), ("gy", 1), ("gz", 2)), 8)
        direct_terms.append(stencil_padded(padded, kernel_taps[level]))
        grid_now = restrict_padded(padded[5:-5, 5:-5, 5:-5])
    block_x, block_y, block_z = grid_now.shape
    copies = jnp.broadcast_to(grid_now.reshape(1, -1, 128), (256, grid_now.size // 128, 128))
    gathered = lax.all_to_all(copies, ("gx", "gy", "gz"), 0, 0)
    count_x, count_y, count_z = (lax.axis_size("gx"), lax.axis_size("gy"), lax.axis_size("gz"))
    whole_grid = gathered.reshape(count_x, count_y, count_z, block_x, block_y, block_z)
    whole_grid = whole_grid.transpose(0, 3, 1, 4, 2, 5).reshape(
        count_x * block_x, count_y * block_y, count_z * block_z
    )
    coarse_list = [whole_grid]
    coarse_list.append(restrict_padded(jnp.pad(coarse_list[-1], 3)))
    coarse_pot = stencil_padded(jnp.pad(coarse_list[-1], 8), kernel_taps[LEVELS - 1])
    level = 3
    coarse_pot = stencil_padded(
        jnp.pad(coarse_list[level - top_level], 8), kernel_taps[level]
    ) + prolong_padded(jnp.pad(coarse_pot, 2))
    padded_pot = jnp.pad(coarse_pot, 2)
    starts = (
        lax.axis_index("gx") * block_x,
        lax.axis_index("gy") * block_y,
        lax.axis_index("gz") * block_z,
    )
    rim_pot = lax.dynamic_slice(padded_pot, starts, (block_x + 4, block_y + 4, block_z + 4))
    current = rim_pot
    for level in range(top_level - 1, -1, -1):
        current = direct_terms[level] + prolong_padded(rim_pot)
        if level > 0:
            rim_pot = extended(current, (("gx", 0), ("gy", 1), ("gz", 2)), 2)
    return current


def solution(mesh):
    in_specs = (P("gx", "gy", "gz"), P())
    out_specs = P("gx", "gy", "gz")
    return jax.shard_map(
        per_device, mesh=mesh, in_specs=in_specs, out_specs=out_specs, check_vma=False
    )
```

```python
import functools
import jax
import jax.numpy as jnp
import numpy as np
from jax import lax
from jax.experimental import pallas as pl
from jax.experimental.pallas import tpu as pltpu
from jax.sharding import PartitionSpec as P

F32, BF16, I32 = jnp.float32, jnp.bfloat16, jnp.int32
CUBIC = (-0.0625, 0.0, 0.5625, 1.0, 0.5625, 0.0, -0.0625)
TAPS_AT = tuple((k - 3, w) for k, w in enumerate(CUBIC) if w != 0.0)

DEVICES = (4, 8, 8)
BX, BY, BZ = (32, 16, 8, 4, 2), (64, 32, 16, 8, 4), (128, 64, 32, 16, 8)
LOW = (0, -1, -2, -2, -2)
EX = (32, 19, 13, 9, 7)
EY = (64, 35, 21, 13, 9)
EZ = (128, 67, 37, 21, 13)
PY = (64, 40, 24, 16, 16)
OZ = (0, 0, 67, 104, 44)
X_SLABS = 9
SECOND = EX[2] - X_SLABS


def inside(level, axis, blocks, cls):
    count = (EX, EY, EZ)[axis][level]
    cells = LOW[level] + np.arange(count)
    ok = np.ones(count, bool)
    if cls == 0:
        ok &= cells >= 0
    if cls == 2:
        ok &= cells < blocks[level]
    return ok


def cubic_matrix(level, axis, blocks, cls):
    ext = (EX, EY, EZ)[axis]
    fine = LOW[level] + np.arange(ext[level])
    coarse = LOW[level + 1] + np.arange(ext[level + 1])
    offset = fine[None, :] - 2 * coarse[:, None]
    matrix = np.zeros(offset.shape)
    for k, w in TAPS_AT:
        matrix[offset == k] = w
    return matrix * inside(level, axis, blocks, cls)[None, :] * inside(level + 1, axis, blocks, cls)[:, None]


def padded(matrix, rows, columns, at_row=0, at_column=0):
    out = np.zeros((rows, columns))
    out[at_row : at_row + matrix.shape[0], at_column : at_column + matrix.shape[1]] = matrix
    return out


def constants():
    out = {}
    for l in range(4):
        out[f"ry{l + 1}"] = np.stack([padded(cubic_matrix(l, 1, BY, c), PY[l + 1], PY[l]) for c in range(3)])
        out[f"py{l}"] = np.stack([padded(cubic_matrix(l, 1, BY, c).T, PY[l], PY[l + 1]) for c in range(3)])
        out[f"rz{l + 1}"] = np.stack(
            [padded(cubic_matrix(l, 2, BZ, c).T, 128, 128, OZ[l], OZ[l + 1]) for c in range(3)]
        )
    for l in range(1, 5):
        mats = []
        for c in range(3):
            m = cubic_matrix(0, 2, BZ, c)
            for k in range(1, l):
                m = cubic_matrix(k, 2, BZ, c) @ m
            mats.append(padded(m, 128, 128))
        out[f"pz{l}"] = np.stack(mats)
    return out


CONSTS = constants()


def split(v):
    hi = v.astype(BF16)
    return hi, (v - hi.astype(F32)).astype(BF16)


def dot(a, b, dims=(((1,), (0,)), ((), ()))):
    return lax.dot_general(a, b, dims, preferred_element_type=F32)


def dot_left_exact(m, b):
    hi, lo = split(b)
    return dot(m, hi) + dot(m, lo)


def dot_right_exact(a, m):
    hi, lo = split(a)
    return dot(hi, m) + dot(lo, m)


def dot3(a, b, dims=(((1,), (0,)), ((), ()))):
    return dot(a[0], b[0], dims) + (dot(a[0], b[1], dims) + dot(a[1], b[0], dims))


def class_of(axis, count):
    i = lax.axis_index(axis)
    return jnp.where(i == 0, 0, jnp.where(i == count - 1, 2, 1))


def x_mask(level, cell):
    i = lax.axis_index("gx")
    if cell < 0:
        return jnp.where(i * BX[level] + cell >= 0, 1.0, 0.0).astype(F32)
    if cell >= BX[level]:
        return jnp.where(i * BX[level] + cell < BX[level] * DEVICES[0], 1.0, 0.0).astype(F32)
    return None


def masked(value, mask):
    return value if mask is None else value * mask


def lanes_mask(first, count):
    lane = lax.broadcasted_iota(I32, (1, 128), 1)
    return (lane >= first) & (lane < first + count)


def restrict_x(level, slab):
    first, last = LOW[level], LOW[level] + EX[level]
    out = []
    for i in range(LOW[level + 1], LOW[level + 1] + EX[level + 1]):
        total = None
        for k, w in TAPS_AT:
            if first <= 2 * i + k < last:
                term = slab(2 * i + k)
                term = term if w == 1.0 else term * w
                total = term if total is None else total + term
        out.append(masked(total, x_mask(level + 1, i)))
    return out


def restrict_kernel(q_ref, *refs):
    names = [f"r{a}{l}" for l in range(1, 5) for a in "yz"]
    mats = dict(zip(names, refs[:8]))
    c1_ref, s1f_ref, s1b_ref, pack_ref = refs[8:12]
    cy, cz = class_of("gy", 8), class_of("gz", 8)
    slab = lambda i: q_ref[i]
    packed = [jnp.zeros((24, 128), F32) for _ in range(X_SLABS)]
    for l in range(1, 5):
        planes = restrict_x(l - 1, slab)
        n, rows = EX[l], PY[l]
        wide = jnp.concatenate(planes, axis=1)
        wide = dot_left_exact(mats[f"ry{l}"][cy], wide)
        tall = jnp.concatenate([wide[:, s * 128 : (s + 1) * 128] for s in range(n)], axis=0)
        tall = dot_right_exact(tall, mats[f"rz{l}"][cz])
        planes = [tall[s * rows : (s + 1) * rows] for s in range(n)]
        if l == 1:
            for s in range(n):
                c1_ref[s] = planes[s]
                if s < 11:
                    s1b_ref[s] = planes[s]
                if s >= n - 11:
                    s1f_ref[s - (n - 11)] = planes[s]
        else:
            for s in range(n):
                value = planes[s]
                if rows < 24:
                    value = jnp.concatenate([value, jnp.zeros((24 - rows, 128), F32)], axis=0)
                if s >= X_SLABS:
                    packed[s - X_SLABS] += pltpu.roll(value, 64, 1)
                else:
                    packed[s] += value
        current = planes
        slab = lambda i, current=current, low=LOW[l]: current[i - low]
    for d in range(4):
        for s in range(X_SLABS):
            pack_ref[d, s] = packed[s]


def conv_x(out_count, taps_ref, level, load, store):
    taps = [taps_ref[level * 51 + t] for t in range(17)]
    for i in range(out_count):
        total = load(i) * taps[0]
        for t in range(1, 17):
            total = total + load(i + t) * taps[t]
        store(i, total)


def x_kernel(taps_ref, q_ref, xl_ref, xr_ref, c1_ref, l1_ref, r1_ref, pack_ref,
             y0_ref, o1_ref, o2_ref, fw_ref, bw_ref, v_ref, q1, g2, g3, g4, o3, o4):
    ix = lax.axis_index("gx")
    taps0 = [taps_ref[t] for t in range(17)]

    def level0(j, _):
        rows = pl.ds(pl.multiple_of(j * 8, 8), 8)
        acc = [None] * 32
        for p in range(48):
            v = xl_ref[p, rows, :] if p < 8 else q_ref[p - 8, rows, :] if p < 40 else xr_ref[p - 40, rows, :]
            for t in range(17):
                i = p - t
                if 0 <= i < 32:
                    term = v * taps0[t]
                    acc[i] = term if acc[i] is None else acc[i] + term
        for i in range(32):
            y0_ref[i, rows, :] = acc[i]
        return 0

    lax.fori_loop(0, 8, level0, 0)
    for i in range(32):
        bw_ref[pl.ds(i * 8, 8), :] = y0_ref[i, pl.ds(0, 8), :]
        fw_ref[pl.ds(i * 8, 8), :] = y0_ref[i, pl.ds(56, 8), :]
    for r in range(35):
        cell = r - 9
        total = None
        for ref, at in ((c1_ref, cell + 1), (l1_ref, cell + 9), (r1_ref, cell - 15)):
            if 0 <= at < ref.shape[0]:
                total = ref[at] if total is None else total + ref[at]
        q1[r] = total

    def keep1(i, total):
        o1_ref[i] = masked(total, x_mask(1, LOW[1] + i))

    conv_x(EX[1], taps_ref, 1, lambda r: q1[r], keep1)
    for level, g in ((2, g2), (3, g3), (4, g4)):
        rows, total_cells = g.shape[1], BX[level] * 4
        g[...] = jnp.zeros_like(g)
        for d in range(4):
            for s in range(EX[level]):
                cell = d * BX[level] + LOW[level] + s
                if not 0 <= cell < total_cells:
                    continue
                if s >= X_SLABS:
                    value = pltpu.roll(pack_ref[d, s - X_SLABS], 64, 1)
                else:
                    value = pack_ref[d, s, pl.ds(0, rows), :]
                g[cell + 10] += value
        out = {2: o2_ref, 3: o3, 4: o4}[level]

        def keep(i, total, out=out, level=level):
            out[i] = masked(total, x_mask(level, LOW[level] + i))

        start = ix * BX[level] + 10 + LOW[level] - 8
        conv_x(EX[level], taps_ref, level, lambda r, g=g, start=start: g[start + r], keep)
    low = lanes_mask(0, EZ[1])
    for s in range(EX[1]):
        f, b = o1_ref[s, pl.ds(24, 16), :], o1_ref[s, pl.ds(0, 16), :]
        if s < EX[2]:
            f = jnp.where(low, f, o2_ref[s, pl.ds(8, 16), :])
            b = jnp.where(low, b, o2_ref[s, pl.ds(0, 16), :])
        fw_ref[pl.ds(256 + s * 16, 16), :] = f
        bw_ref[pl.ds(256 + s * 16, 16), :] = b
    columns = []
    for level, o, members in ((3, o3, range(0, 5)), (3, o3, range(5, 9)), (4, o4, range(0, 7))):
        mask = lanes_mask(OZ[level], EZ[level])
        total = jnp.zeros((16, 128), F32)
        for n, s in enumerate(members):
            value = jnp.where(mask, o[s], 0.0)
            total = total + pltpu.roll(value, (n * EZ[level] - OZ[level]) % 128, 1)
        columns.append(total)
    for d in range(8):
        for c in range(3):
            v_ref[d, :, pl.ds(c * 128, 128)] = columns[c]


def toeplitz(taps_ref, level, axis, diff):
    total = jnp.zeros(diff.shape, F32)
    for t in range(17):
        total = jnp.where(diff == t, taps_ref[level * 51 + axis * 17 + t], total)
    return total


def store_split(refs, value, rows=None):
    hi, lo = split(value)
    if rows is None:
        refs[0][...] = hi
        refs[1][...] = lo
    else:
        refs[0][rows, :] = hi
        refs[1][rows, :] = lo


def prep_kernel(taps_ref, pz1, pz2, pz3, pz4, *out):
    iy = lax.axis_index("gy")
    cz = class_of("gz", 8)
    iz = lax.axis_index("gz")
    bad = 1000
    iota = lambda shape, d: lax.broadcasted_iota(I32, shape, d)
    outs = [out[2 * k : 2 * k + 2] for k in range(10)]

    def out_cells(level, blocks, ext, index, position, count):
        cell = index + LOW[level]
        g = cell + position * blocks[level]
        ok = (index < ext[level]) & (g >= 0) & (g < blocks[level] * count)
        return jnp.where(ok, cell, -bad)

    for level, width, ref in ((0, 80, outs[0]), (1, 72, outs[1]), (2, 56, outs[2])):
        shape = (PY[level], width)
        i, j = iota(shape, 0), iota(shape, 1)
        to = out_cells(level, BY, EY, i, iy, 8)
        if level == 0:
            at = j - 8
        else:
            halo, reach = 16, 11 if level == 1 else 13
            own = j - halo
            upper = own - PY[level]
            lowest = LOW[level] - 8
            at = jnp.where(
                own < 0,
                jnp.where(j < reach, j + lowest, bad),
                jnp.where(
                    upper < 0,
                    jnp.where(own < EY[level], own + LOW[level], bad),
                    jnp.where(upper < reach, upper + LOW[level] + BY[level], bad),
                ),
            )
        store_split(ref, toeplitz(taps_ref, level, 1, at - to + 8))
    for level, ref in ((3, outs[3]), (4, outs[4])):
        i, j = iota((16, 128), 0), iota((16, 128), 1)
        to = out_cells(level, BY, EY, i, iy, 8)
        d, r = j // 16, j % 16
        at = jnp.where(r < EY[level], (d - iy) * BY[level] + r + LOW[level], bad)
        store_split(ref, toeplitz(taps_ref, level, 1, at - to + 8))
    j = iota((128, 128), 0)
    c = iota((128, 128), 1)
    store_split(outs[5], toeplitz(taps_ref, 0, 2, j - c + 8), pl.ds(0, 128))
    j, c = iota((16, 128), 0), iota((16, 128), 1)
    store_split(outs[5], toeplitz(taps_ref, 0, 2, jnp.where(j < 8, j - 8, j - 8 + 128) - c + 8), pl.ds(128, 16))
    for level, pz, ref in ((1, pz1, outs[6]), (2, pz2, outs[7]), (3, pz3, outs[8]), (4, pz4, outs[9])):
        prolong = split(pz[cz])
        c = iota((128, 128), 1)
        to = out_cells(level, BZ, EZ, c, iz, 8)
        j = iota((128, 128), 0) - OZ[level]
        at = jnp.where((j >= 0) & (j < EZ[level]), j + LOW[level], bad)
        store_split(ref, dot3(split(toeplitz(taps_ref, level, 2, at - to + 8)), prolong), pl.ds(0, 128))
        rows = 64 if level == 4 else 32
        c = iota((rows, 128), 1)
        to = out_cells(level, BZ, EZ, c, iz, 8)
        j = iota((rows, 128), 0)
        r = j % 16
        if level == 4:
            d = j // 16
            shift = jnp.where(d == 0, -2, jnp.where(d == 1, -1, jnp.where(d == 2, 1, 2))) * BZ[4]
            at = jnp.where(r < EZ[4], shift + r + LOW[4], bad)
        else:
            reach = 11 if level == 1 else 13
            at = jnp.where(j < 16, r + LOW[level] - 8, r + LOW[level] + BZ[level])
            at = jnp.where(r < reach, at, bad)
        store_split(ref, dot3(split(toeplitz(taps_ref, level, 2, at - to + 8)), prolong), pl.ds(128, rows))


def y_kernel(y0_ref, o1_ref, o2_ref, lo_ref, hi_ref, v_ref, *refs):
    my = [(refs[2 * k], refs[2 * k + 1]) for k in range(5)]
    z0_ref, z1_ref, z2_ref, z3_ref, z4_ref, fw_ref, bw_ref, t4_ref = refs[10:]
    m0 = (my[0][0][...], my[0][1][...])
    for base in range(0, 32, 4):
        parts = []
        for i in range(base, base + 4):
            parts.append(jnp.concatenate(
                [lo_ref[pl.ds(i * 8, 8), :], y0_ref[i], hi_ref[pl.ds(i * 8, 8), :]], axis=0))
        out = dot3(m0, split(jnp.concatenate(parts, axis=1)))
        for n in range(4):
            z0_ref[pl.ds((base + n) * 64, 64), :] = out[:, n * 128 : (n + 1) * 128]
    for level, o_ref, z_ref in ((1, o1_ref, z1_ref), (2, o2_ref, z2_ref)):
        m = (my[level][0][...], my[level][1][...])
        n, rows = EX[level], PY[level]
        parts = [jnp.concatenate([lo_ref[pl.ds(256 + s * 16, 16), :], o_ref[s], hi_ref[pl.ds(256 + s * 16, 16), :]], axis=0)
                 for s in range(n)]
        out = dot3(m, split(jnp.concatenate(parts, axis=1)))
        for s in range(n):
            z_ref[pl.ds(s * rows, rows), :] = out[:, s * 128 : (s + 1) * 128]
    everything = jnp.concatenate([v_ref[d] for d in range(8)], axis=0)
    pair = split(everything)
    o3 = dot3((my[3][0][...], my[3][1][...]), (pair[0][:, :256], pair[1][:, :256]))
    o4 = dot3((my[4][0][...], my[4][1][...]), (pair[0][:, 256:], pair[1][:, 256:]))
    for level, source, members, z_ref in (
        (3, o3[:, :128], range(0, 5), z3_ref), (3, o3[:, 128:], range(5, 9), z3_ref), (4, o4, range(0, 7), z4_ref)
    ):
        for n, s in enumerate(members):
            z_ref[pl.ds(s * 16, 16), :] = pltpu.roll(source, (OZ[level] - n * EZ[level]) % 128, 1)
    for k in range(16):
        t = z0_ref[pl.ds(k * 128, 128), :].T
        bw_ref[pl.ds(0, 8), pl.ds(k * 128, 128)] = t[:8]
        fw_ref[pl.ds(0, 8), pl.ds(k * 128, 128)] = t[120:]
    for k in range(6):
        size = 128 if k < 5 else 120
        block = z1_ref[pl.ds(k * 128, size), :]
        if size < 128:
            block = jnp.concatenate([block, jnp.zeros((128 - size, 128), F32)], axis=0)
        t = block.T
        bw_ref[pl.ds(8, 16), pl.ds(k * 128, 128)] = t[0:16]
        fw_ref[pl.ds(8, 16), pl.ds(k * 128, 128)] = t[56:72]
    for level, z_ref, at, f, count in ((2, z2_ref, 768, 24, 312), (3, z3_ref, 1152, 8, 144)):
        for k in range((count + 127) // 128):
            size = min(128, count - k * 128)
            block = pltpu.roll(z_ref[pl.ds(k * 128, size), :], (-OZ[level]) % 128, 1)
            if size < 128:
                block = jnp.concatenate([block, jnp.zeros((128 - size, 128), F32)], axis=0)
            t = block.T
            bw_ref[pl.ds(8, 16), pl.ds(at + k * 128, 128)] = t[0:16]
            fw_ref[pl.ds(8, 16), pl.ds(at + k * 128, 128)] = t[f : f + 16]
    block = pltpu.roll(z4_ref[...], (-OZ[4]) % 128, 1)
    t = jnp.concatenate([block, jnp.zeros((16, 128), F32)], axis=0).T[:16]
    for ref in (bw_ref, fw_ref):
        ref[pl.ds(8, 16), pl.ds(1408, 128)] = t
    t4_ref[...] = t


def z_kernel(z0_ref, z1_ref, z2_ref, z3_ref, z4_ref, lo_ref, hi_ref, l4_ref, h4_ref, *refs):
    mz = [(refs[2 * k], refs[2 * k + 1]) for k in range(5)]
    py = refs[10:14]
    out_ref = refs[14]
    acc = refs[15]
    cy = class_of("gy", 8)
    first = (((0,), (0,)), ((), ()))

    def level_out(level, own, halo, rows_own=128):
        a, b = mz[level]
        k = halo.shape[0]
        return dot3(split(own), (a[pl.ds(0, 128), :], b[pl.ds(0, 128), :])) + dot3(
            split(halo), (a[pl.ds(128, k), :], b[pl.ds(128, k), :]), first)

    at = {1: 0, 2: 768, 3: 1152, 4: 1408}
    rows = {1: 760, 2: 312, 3: 144, 4: 112}
    z_refs = {1: z1_ref, 2: z2_ref, 3: z3_ref, 4: z4_ref}
    total = None
    for level in (4, 3, 2, 1):
        n = rows[level]
        columns = pl.ds(at[level], (n + 127) // 128 * 128)
        if level == 4:
            halo = jnp.concatenate([l4_ref[...], lo_ref[pl.ds(8, 16), columns], hi_ref[pl.ds(8, 16), columns], h4_ref[...]], axis=0)
        else:
            halo = jnp.concatenate([lo_ref[pl.ds(8, 16), columns], hi_ref[pl.ds(8, 16), columns]], axis=0)
        full = (n + 127) // 128 * 128
        own = z_refs[level][...]
        if full > n:
            own = jnp.concatenate([own, jnp.zeros((full - n, 128), F32)], axis=0)
        term = level_out(level, own, halo)
        planes = [term[s * PY[level] : (s + 1) * PY[level]] for s in range(EX[level])]
        if total is not None:
            planes = [a + b for a, b in zip(planes, total)]
        fine = level - 1
        wide = dot_left_exact(py[fine][cy], jnp.concatenate(planes, axis=1))
        coarse = [wide[:, s * 128 : (s + 1) * 128] for s in range(EX[level])]
        total = []
        for cell in range(LOW[fine], LOW[fine] + EX[fine]):
            value = None
            for k, w in TAPS_AT:
                if (cell - k) % 2 == 0:
                    s = (cell - k) // 2 - LOW[level]
                    if 0 <= s < EX[level]:
                        term = coarse[s] if w == 1.0 else coarse[s] * w
                        value = term if value is None else value + term
            value = masked(value, x_mask(fine, cell)) if fine else value
            total.append(value)
            if fine == 0:
                acc[cell] = value
    halo = jnp.concatenate([lo_ref[pl.ds(0, 8), :], hi_ref[pl.ds(0, 8), :]], axis=0)
    for k in range(4):
        term = level_out(0, z0_ref[pl.ds(k * 512, 512), :], halo[:, k * 512 : (k + 1) * 512])
        for i in range(8):
            out_ref[k * 8 + i] = acc[k * 8 + i] + term[i * 64 : (i + 1) * 64]


VM = pl.BlockSpec(memory_space=pltpu.VMEM)
SM = pl.BlockSpec(memory_space=pltpu.SMEM)


def call(body, name, shapes, in_specs, scratch=(), flops=10**8):
    return pl.pallas_call(
        body,
        name=name,
        out_shape=[jax.ShapeDtypeStruct(s, d) for s, d in shapes],
        in_specs=in_specs,
        out_specs=[VM] * len(shapes),
        scratch_shapes=list(scratch),
        cost_estimate=pl.CostEstimate(flops=flops, bytes_accessed=2**21, transcendentals=0),
    )


def steps(axis, by):
    count = lax.axis_size(axis)
    return [(i, i + by) for i in range(count) if 0 <= i + by < count]


def per_device(charges, kernel_taps):
    taps = kernel_taps.reshape(-1)
    shift = lambda v, axis, by: lax.ppermute(v, axis, steps(axis, by))
    const = {k: jnp.asarray(v, F32 if k.startswith("pz") else BF16) for k, v in CONSTS.items()}
    xl = shift(charges[24:], "gx", 1)
    xr = shift(charges[:8], "gx", -1)
    c1, s1f, s1b, pack = call(
        restrict_kernel, "restrict",
        [((19, 40, 128), F32), ((11, 40, 128), F32), ((11, 40, 128), F32), ((4, X_SLABS, 24, 128), F32)],
        [VM] * 9,
    )(charges, *[const[f"r{a}{l}"] for l in range(1, 5) for a in "yz"])
    l1 = shift(s1f, "gx", 1)
    r1 = shift(s1b, "gx", -1)
    packs = lax.all_to_all(pack, "gx", 0, 0)
    widths = [(64, 80), (40, 72), (24, 56), (16, 128), (16, 128), (144, 128), (160, 128), (160, 128), (160, 128), (192, 128)]
    mats = call(
        prep_kernel, "prep", [(w, BF16) for w in widths for _ in range(2)], [SM] + [VM] * 4
    )(taps, *[const[f"pz{l}"] for l in range(1, 5)])
    y0, o1, o2, fw, bw, v = call(
        x_kernel, "alongx",
        [((32, 64, 128), F32), ((19, 40, 128), F32), ((13, 24, 128), F32), ((560, 128), F32), ((560, 128), F32),
         ((8, 16, 384), F32)],
        [SM] + [VM] * 7,
        [pltpu.VMEM((35, 40, 128), F32), pltpu.VMEM((53, 24, 128), F32), pltpu.VMEM((37, 16, 128), F32),
         pltpu.VMEM((29, 16, 128), F32), pltpu.VMEM((9, 16, 128), F32), pltpu.VMEM((7, 16, 128), F32)],
    )(taps, charges, xl, xr, c1, l1, r1, packs)
    lo = shift(fw, "gy", 1)
    hi = shift(bw, "gy", -1)
    vs = lax.all_to_all(v, "gy", 0, 0)
    z0, z1, z2, z3, z4, fw, bw, t4 = call(
        y_kernel, "alongy",
        [((2048, 128), F32), ((760, 128), F32), ((312, 128), F32), ((144, 128), F32), ((112, 128), F32),
         ((24, 2048), F32), ((24, 2048), F32), ((16, 128), F32)],
        [VM] * 16,
    )(y0, o1, o2, lo, hi, vs, *mats[:10])
    lo = shift(fw, "gz", 1)
    hi = shift(bw, "gz", -1)
    l4 = shift(t4, "gz", 2)
    h4 = shift(t4, "gz", -2)
    (out,) = call(
        z_kernel, "alongz", [((32, 64, 128), F32)], [VM] * 23, [pltpu.VMEM((32, 64, 128), F32)]
    )(z0, z1, z2, z3, z4, lo, hi, l4, h4, *mats[10:], *[const[f"py{l}"] for l in range(4)])
    return out


def solution(mesh):
    return jax.shard_map(
        per_device,
        mesh=mesh,
        in_specs=(P("gx", "gy", "gz"), P()),
        out_specs=P("gx", "gy", "gz"),
        check_vma=False,
    )
```

```python
import jax
import jax.numpy as jnp
from jax import lax
from jax.experimental import pallas as pl
from jax.experimental.pallas import tpu as pltpu
from jax.sharding import PartitionSpec as P


F32, BF16, I32 = jnp.float32, jnp.bfloat16, jnp.int32
CUBIC = (-0.0625, 0.0, 0.5625, 1.0, 0.5625, 0.0, -0.0625)
TAPS_AT = tuple((k - 3, w) for k, w in enumerate(CUBIC) if w != 0.0)

DEVICES = (4, 8, 8)
BX, BY, BZ = (32, 16, 8, 4, 2), (64, 32, 16, 8, 4), (128, 64, 32, 16, 8)
LOW = (0, -1, -2, -2, -2)
EX = (32, 19, 13, 9, 7)
EY = (64, 35, 21, 13, 9)
EZ = (128, 67, 37, 21, 13)
PY = (64, 40, 24, 16, 16)
OZ = (0, 0, 67, 104, 44)
FAR = (range(0, 3), range(3, 5))
V_COLUMNS = ((3, range(0, 5)), (3, range(5, 9)), (4, range(0, 7)))


def up16(n):
    return (n + 15) // 16 * 16


def iota(shape, dim):
    return lax.broadcasted_iota(I32, shape, dim)


def in_grid(level, ext, blocks, count, index, position):
    cell = index + LOW[level]
    g = cell + position * blocks[level]
    return (index >= 0) & (index < ext[level]) & (g >= 0) & (g < blocks[level] * count)


def cubic_matrix(level, ext, blocks, count, position, fine, coarse):
    offset = fine + LOW[level] - 2 * (coarse + LOW[level + 1])
    value = jnp.zeros(offset.shape, F32)
    for k, w in TAPS_AT:
        value = jnp.where(offset == k, w, value)
    ok = in_grid(level, ext, blocks, count, fine, position) & in_grid(level + 1, ext, blocks, count, coarse, position)
    return jnp.where(ok, value, 0.0)


def repeated(index, period):
    for _ in range(2):
        index = jnp.where(index >= period, index - period, index)
    return index


def restrict_y(level, position):
    half = up16(PY[level])
    shape = (PY[level + 1], 2 * half)
    return cubic_matrix(level, EY, BY, 8, position, repeated(iota(shape, 1), half), iota(shape, 0)).astype(BF16)


def prolong_y(level, position):
    half = up16(PY[level + 1])
    shape = (PY[level], 2 * half)
    return cubic_matrix(level, EY, BY, 8, position, iota(shape, 0), repeated(iota(shape, 1), half)).astype(BF16)


def restrict_z(level, position):
    shape = (128, 128)
    m = cubic_matrix(level, EZ, BZ, 8, position, iota(shape, 0) - OZ[level], iota(shape, 1) - OZ[level + 1]).astype(BF16)
    return jnp.concatenate([m, m], axis=0)


def split(v):
    hi = v.astype(BF16)
    return hi, (v - hi.astype(F32)).astype(BF16)


def dot(a, b, dims=(((1,), (0,)), ((), ()))):
    return lax.dot_general(a, b, dims, preferred_element_type=F32)


def stacked(value, *order):
    rows = up16(value.shape[0])
    if rows > value.shape[0]:
        value = jnp.concatenate([value, jnp.zeros((rows - value.shape[0], value.shape[1]), F32)], axis=0)
    parts = split(value)
    return jnp.concatenate([parts[k] for k in order], axis=0)


def dot_left_exact(m, b):
    return dot(m, stacked(b, 0, 1))


def dot_right_exact(a, m):
    return dot(jnp.concatenate(split(a), axis=1), m)


def dot3(a, b, dims=(((1,), (0,)), ((), ()))):
    return dot(a[0], b[0], dims) + (dot(a[0], b[1], dims) + dot(a[1], b[0], dims))


def x_mask(level, cell):
    i = lax.axis_index("gx")
    if cell < 0:
        return jnp.where(i * BX[level] + cell >= 0, 1.0, 0.0).astype(F32)
    if cell >= BX[level]:
        return jnp.where(i * BX[level] + cell < BX[level] * DEVICES[0], 1.0, 0.0).astype(F32)
    return None


def masked(value, mask):
    return value if mask is None else value * mask


def lanes_mask(first, count):
    lane = lax.broadcasted_iota(I32, (1, 128), 1)
    return (lane >= first) & (lane < first + count)


def restrict_x(level, slab):
    first, last = LOW[level], LOW[level] + EX[level]
    out = []
    for i in range(LOW[level + 1], LOW[level + 1] + EX[level + 1]):
        total = None
        for k, w in TAPS_AT:
            if first <= 2 * i + k < last:
                term = slab(2 * i + k)
                term = term if w == 1.0 else term * w
                total = term if total is None else total + term
        out.append(masked(total, x_mask(level + 1, i)))
    return out


def restrict_kernel(q_ref, s1f_ref, s1b_ref, s2_ref, v_ref, far):
    for s in range(8):
        s1b_ref[pl.ds(s * 64, 64), :] = q_ref[s]
        s1f_ref[pl.ds(s * 64, 64), :] = q_ref[s + 24]
    ix, iy, iz = lax.axis_index("gx"), lax.axis_index("gy"), lax.axis_index("gz")
    low = lanes_mask(0, EZ[1])
    slab = lambda i: q_ref[i]
    kept = {}
    for l in range(1, 5):
        planes = restrict_x(l - 1, slab)
        n, rows = EX[l], PY[l]
        wide = jnp.concatenate(planes, axis=1)
        wide = dot_left_exact(restrict_y(l - 1, iy), wide)
        tall = jnp.concatenate([wide[:, s * 128 : (s + 1) * 128] for s in range(n)], axis=0)
        tall = dot_right_exact(tall, restrict_z(l - 1, iz))
        planes = kept[l] = [tall[s * rows : (s + 1) * rows] for s in range(n)]
        slab = lambda i, planes=planes, low=LOW[l]: planes[i - low]
    for s in range(EX[2]):
        far[s] = kept[2][s]
    for s in range(11):
        for ref, at in ((s1b_ref, s), (s1f_ref, s + EX[1] - 11)):
            ref[pl.ds(512 + s * 40, 24), :] = jnp.where(low, kept[1][at][:24], kept[2][s])
            ref[pl.ds(512 + s * 40 + 24, 16), :] = kept[1][at][24:]
    for s in range(11, EX[2]):
        for ref in (s1b_ref, s1f_ref):
            ref[pl.ds(952 + (s - 11) * 24, 24), :] = kept[2][s]
    start = jnp.where(ix < 2, 8, 0)
    mask = lanes_mask(OZ[2], EZ[2])
    for k, members in enumerate(FAR):
        total = jnp.zeros((24, 128), F32)
        for n, s in enumerate(members):
            total = total + pltpu.roll(jnp.where(mask, far[start + s], 0.0), (n * EZ[2] - OZ[2]) % 128, 1)
        s2_ref[k] = total
    for c, (level, members) in enumerate(V_COLUMNS):
        mask = lanes_mask(OZ[level], EZ[level])
        total = jnp.zeros((16, 128), F32)
        for n, s in enumerate(members):
            value = jnp.where(mask, kept[level][s], 0.0)
            total = total + pltpu.roll(value, (n * EZ[level] - OZ[level]) % 128, 1)
        for d in range(8):
            v_ref[d, :, pl.ds(c * 128, 128)] = total


def conv_x(out_count, taps_ref, level, load, store):
    if len(taps_ref.shape) == 3:
        taps = [taps_ref[level, 0, t] for t in range(17)]
    else:
        taps = [taps_ref[pl.ds((level - 3) * 24 + t, 1), :] for t in range(17)]
    for i in range(out_count):
        total = load(i) * taps[0]
        for t in range(1, 17):
            total = total + load(i + t) * taps[t]
        store(i, total)


def x_kernel(taps_ref, q_ref, sf_ref, sb_ref, l_ref, r_ref, f_ref, y0_ref, o_ref, fw_ref, bw_ref, tb_ref, q1, q2):
    ix = lax.axis_index("gx")
    taps0 = [taps_ref[0, 0, t] for t in range(17)]

    def level0(j, _):
        rows = pl.ds(pl.multiple_of(j * 8, 8), 8)
        for first in (0, 16):
            acc = {}
            for p in range(first, first + 32):
                if p < 8:
                    v = l_ref[pl.ds(pl.multiple_of(p * 64 + j * 8, 8), 8), :]
                elif p < 40:
                    v = q_ref[p - 8, rows, :]
                else:
                    v = r_ref[pl.ds(pl.multiple_of((p - 40) * 64 + j * 8, 8), 8), :]
                for t in range(17):
                    i = p - t
                    if first <= i < first + 16:
                        term = v * taps0[t]
                        acc[i] = acc[i] + term if i in acc else term
            for i, value in acc.items():
                y0_ref[i, rows, :] = value
        return 0

    lax.fori_loop(0, 8, level0, 0)
    for i in range(32):
        bw_ref[pl.ds(i * 8, 8), :] = y0_ref[i, pl.ds(0, 8), :]
        fw_ref[pl.ds(i * 8, 8), :] = y0_ref[i, pl.ds(56, 8), :]

    def received(ref, at, rows):
        if not 0 <= at < (11 if rows == 40 else 13):
            return None
        return ref[pl.ds(512 + at * 40 if at < 11 else 952 + (at - 11) * 24, rows), :]

    def added(values):
        values = [v for v in values if v is not None]
        total = values[0]
        for v in values[1:]:
            total = total + v
        return total

    def own(at, rows):
        if rows == 24 or at < 11:
            return received(sb_ref, at, rows)
        return received(sf_ref, at - 8, rows)

    for r in range(35):
        cell = r - 9
        q1[r] = added([own(cell + 1, 40), received(l_ref, cell + 9, 40), received(r_ref, cell - 15, 40)])
    for r in range(29):
        cell = r - 10
        q2[r] = added([own(cell + 2, 24), received(l_ref, cell + 10, 24), received(r_ref, cell - 6, 24)])
    start = jnp.where(ix < 2, 24, 0)
    mask = lanes_mask(OZ[2], EZ[2])
    for k, members in enumerate(FAR):
        for n, s in enumerate(members):
            q2[start + s] += jnp.where(mask, pltpu.roll(f_ref[pl.ds(48 + k * 24, 24), :], (OZ[2] - n * EZ[2]) % 128, 1), 0.0)
    low = lanes_mask(0, EZ[1])
    two = {}

    def keep2(i, total):
        two[i] = masked(total, x_mask(2, LOW[2] + i))

    def keep1(s, total):
        total = masked(total, x_mask(1, LOW[1] + s))
        f, b = total[24:40], total[:16]
        o_ref[s, pl.ds(24, 16), :] = f
        o_ref[s, pl.ds(0, 24), :] = jnp.where(low, total[:24], two[s]) if s < EX[2] else total[:24]
        if s < EX[2]:
            f = jnp.where(low, f, two[s][8:])
            b = jnp.where(low, b, two[s][:16])
        fw_ref[pl.ds(256 + s * 16, 16), :] = f
        bw_ref[pl.ds(256 + s * 16, 16), :] = b

    for level in (3, 4):
        for t in range(17):
            tb_ref[pl.ds((level - 3) * 24 + t, 1), :] = jnp.full((1, 128), taps_ref[level, 0, t], F32)
    conv_x(EX[2], taps_ref, 2, lambda r: q2[r], keep2)
    conv_x(EX[1], taps_ref, 1, lambda r: q1[r], keep1)


def coarse_y_kernel(taps_ref, v_ref, s2_ref, near_ref, far_ref):
    iy = lax.axis_index("gy")
    block = stacked(jnp.concatenate([v_ref[k] for k in range(8)], axis=0), 0, 1, 0)
    for level, first, last in ((3, 0, 256), (4, 256, 384)):
        i, j = iota((16, 384), 0), iota((16, 384), 1) & 127
        to = out_cells(level, BY, EY, i, iy, 8)
        d, r = j >> 4, j & 15
        at = jnp.where(r < EY[level], (d - iy) * BY[level] + r + LOW[level], BAD)
        out = dot(thirds(toeplitz(taps_ref, level, 1, at - to + 8), 128), block[:, first:last])
        for c in range(first, last, 128):
            for ref in (near_ref, far_ref):
                ref[pl.ds(c // 8, 16), :] = out[:, c - first : c - first + 128]
    for k in range(2):
        far_ref[pl.ds(48 + k * 24, 24), :] = s2_ref[k]


def coarse_kernel(taps_ref, own_ref, low_ref, high_ref, far_ref, z3_ref, z4_ref, t4_ref, g3, g4):
    ix = lax.axis_index("gx")
    for g in (g3, g4):
        g[...] = jnp.zeros_like(g)
    for ref, step in ((own_ref, 0), (low_ref, 3), (high_ref, 1), (far_ref, 2)):
        source = (ix + step) & 3
        for c, (level, members) in enumerate(V_COLUMNS):
            g = g3 if level == 3 else g4
            column = ref[pl.ds(c * 16, 16), :]
            for n, s in enumerate(members):
                g[source * BX[level] + (LOW[level] + s + 10)] += pltpu.roll(column, (OZ[level] - n * EZ[level]) % 128, 1)
    for level, g, z_ref in ((3, g3, z3_ref), (4, g4, z4_ref)):
        start = ix * BX[level] + 10 + LOW[level] - 8

        def keep(i, total, level=level, z_ref=z_ref):
            z_ref[pl.ds(i * 16, 16), :] = masked(total, x_mask(level, LOW[level] + i))

        conv_x(EX[level], taps_ref, level, lambda r, g=g, start=start: g[start + r], keep)
    t4_ref[...] = level4_rows(z4_ref)


BAD = 1000


def out_cells(level, blocks, ext, index, position, count):
    return jnp.where(in_grid(level, ext, blocks, count, index, position), index + LOW[level], -BAD)


def thirds(value, third):
    hi, lo = split(value)
    return jnp.where(iota(value.shape, 1) < 2 * third, hi.astype(F32), lo.astype(F32)).astype(BF16)


def toeplitz(taps_ref, level, axis, diff):
    total = jnp.zeros(diff.shape, F32)
    for t in range(17):
        total = jnp.where(diff == t, taps_ref[level, axis, t], total)
    return total


def store_z(ref, halo_ref, own, halo):
    ref[...] = jnp.concatenate(split(own), axis=1)
    hi, lo = split(halo)
    halo_ref[...] = jnp.concatenate([hi, hi, lo], axis=0)


def prep_kernel(taps_ref, *out):
    iy = lax.axis_index("gy")
    iz = lax.axis_index("gz")
    outs = out[:3]
    z_outs = [out[3 + 2 * k : 5 + 2 * k] for k in range(5)]

    for level, width, ref in ((0, 80, outs[0]), (1, 80, outs[1]), (2, 64, outs[2])):
        shape = (PY[level], 3 * width)
        i, j = iota(shape, 0), repeated(iota(shape, 1), width)
        to = out_cells(level, BY, EY, i, iy, 8)
        if level == 0:
            at = j - 8
        else:
            halo, reach = 16, 11 if level == 1 else 13
            own = j - halo
            upper = own - PY[level]
            lowest = LOW[level] - 8
            at = jnp.where(
                own < 0,
                jnp.where(j < reach, j + lowest, BAD),
                jnp.where(
                    upper < 0,
                    jnp.where(own < EY[level], own + LOW[level], BAD),
                    jnp.where(upper < reach, upper + LOW[level] + BY[level], BAD),
                ),
            )
        ref[...] = thirds(toeplitz(taps_ref, level, 1, at - to + 8), width)
    j = iota((128, 128), 0)
    c = iota((128, 128), 1)
    own = toeplitz(taps_ref, 0, 2, j - c + 8)
    j, c = iota((16, 128), 0), iota((16, 128), 1)
    store_z(*z_outs[0], own, toeplitz(taps_ref, 0, 2, jnp.where(j < 8, j - 8, j - 8 + 128) - c + 8))
    for level in range(4):
        out[13 + level][...] = prolong_y(level, iy)
    prolong = None
    for level in range(1, 5):
        shape = (128, 128)
        one = cubic_matrix(level - 1, EZ, BZ, 8, iz, iota(shape, 1), iota(shape, 0)).astype(BF16)
        whole = one.astype(F32) if prolong is None else dot(one, prolong[0]) + dot(one, prolong[1])
        prolong = split(whole)
        c = iota((128, 128), 1)
        to = out_cells(level, BZ, EZ, c, iz, 8)
        j = iota((128, 128), 0) - OZ[level]
        at = jnp.where((j >= 0) & (j < EZ[level]), j + LOW[level], BAD)
        own = dot3(split(toeplitz(taps_ref, level, 2, at - to + 8)), prolong)
        rows = 64 if level == 4 else 32
        c = iota((rows, 128), 1)
        to = out_cells(level, BZ, EZ, c, iz, 8)
        j = iota((rows, 128), 0)
        r = j & 15
        if level == 4:
            d = j >> 4
            shift = jnp.where(d == 0, -2, jnp.where(d == 1, -1, jnp.where(d == 2, 1, 2))) * BZ[4]
            at = jnp.where(r < EZ[4], shift + r + LOW[4], BAD)
        else:
            reach = 11 if level == 1 else 13
            at = jnp.where(j < 16, r + LOW[level] - 8, r + LOW[level] + BZ[level])
            at = jnp.where(r < reach, at, BAD)
        store_z(*z_outs[level], own, dot3(split(toeplitz(taps_ref, level, 2, at - to + 8)), prolong))


def level4_rows(z4_ref):
    block = pltpu.roll(z4_ref[...], (-OZ[4]) % 128, 1)
    return jnp.concatenate([block, jnp.zeros((16, 128), F32)], axis=0).T[:16]


def y_kernel(y0_ref, o_ref, lo_ref, hi_ref, z3_ref, z4_ref, *refs):
    my = [ref[...] for ref in refs[:3]]
    z0_ref, z1_ref, z2_ref, fw_ref, bw_ref = refs[3:]
    for base in range(0, 32, 4):
        parts = []
        for i in range(base, base + 4):
            parts.append(jnp.concatenate(
                [lo_ref[pl.ds(i * 8, 8), :], y0_ref[i], hi_ref[pl.ds(i * 8, 8), :]], axis=0))
        out = dot(my[0], stacked(jnp.concatenate(parts, axis=1), 0, 1, 0))
        for n in range(4):
            z0_ref[pl.ds((base + n) * 64, 64), :] = out[:, n * 128 : (n + 1) * 128]
    for level, z_ref in ((1, z1_ref), (2, z2_ref)):
        n, rows = EX[level], PY[level]
        parts = [jnp.concatenate([lo_ref[pl.ds(256 + s * 16, 16), :], o_ref[s, pl.ds(0, rows), :], hi_ref[pl.ds(256 + s * 16, 16), :]], axis=0)
                 for s in range(n)]
        out = dot(my[level], stacked(jnp.concatenate(parts, axis=1), 0, 1, 0))
        for s in range(n):
            z_ref[pl.ds(s * rows, rows), :] = out[:, s * 128 : (s + 1) * 128]
    for k in range(16):
        t = z0_ref[pl.ds(k * 128, 128), :].T
        bw_ref[pl.ds(0, 8), pl.ds(k * 128, 128)] = t[:8]
        fw_ref[pl.ds(0, 8), pl.ds(k * 128, 128)] = t[120:]
    for k in range(6):
        size = 128 if k < 5 else 120
        block = z1_ref[pl.ds(k * 128, size), :]
        if size < 128:
            block = jnp.concatenate([block, jnp.zeros((128 - size, 128), F32)], axis=0)
        t = block.T
        bw_ref[pl.ds(8, 16), pl.ds(k * 128, 128)] = t[0:16]
        fw_ref[pl.ds(8, 16), pl.ds(k * 128, 128)] = t[56:72]
    for level, z_ref, at, f, count in ((2, z2_ref, 768, 24, 312), (3, z3_ref, 1152, 8, 144)):
        for k in range((count + 127) // 128):
            size = min(128, count - k * 128)
            block = pltpu.roll(z_ref[pl.ds(k * 128, size), :], (-OZ[level]) % 128, 1)
            if size < 128:
                block = jnp.concatenate([block, jnp.zeros((128 - size, 128), F32)], axis=0)
            t = block.T
            bw_ref[pl.ds(8, 16), pl.ds(at + k * 128, 128)] = t[0:16]
            fw_ref[pl.ds(8, 16), pl.ds(at + k * 128, 128)] = t[f : f + 16]
    t = level4_rows(z4_ref)
    for ref in (bw_ref, fw_ref):
        ref[pl.ds(8, 16), pl.ds(1408, 128)] = t


Z_AT = {0: 0, 1: 0, 2: 768, 3: 1152, 4: 1408}
Z_ROWS = {0: 2048, 1: 760, 2: 312, 3: 144, 4: 112}


def own_kernel(*refs):
    for level in range(5):
        z_ref, m_ref, t_ref = refs[level], refs[5 + level], refs[10 + level]
        m = m_ref[...]
        m = jnp.concatenate([m, jnp.concatenate([m[:, :128], jnp.zeros((128, 128), BF16)], axis=1)], axis=0)
        step = 512 if level == 0 else Z_ROWS[level]
        for k in range(0, Z_ROWS[level], step):
            both = dot(jnp.concatenate(split(z_ref[pl.ds(k, step), :]), axis=1), m)
            t_ref[pl.ds(k, step), :] = both[:, :128] + both[:, 128:]


def z_kernel(*refs):
    t_refs, (lo_ref, hi_ref, l4_ref, h4_ref), m_refs, py = refs[:5], refs[5:9], refs[9:14], refs[14:18]
    out_ref, acc = refs[18:]
    first = (((0,), (0,)), ((), ()))

    def halo_part(level, halo):
        return dot(stacked(halo, 0, 1, 0), m_refs[level][...], first)

    total = None
    for level in (4, 3, 2, 1):
        n = Z_ROWS[level]
        columns = pl.ds(Z_AT[level], (n + 127) // 128 * 128)
        halo = [lo_ref[pl.ds(8, 16), columns], hi_ref[pl.ds(8, 16), columns]]
        if level == 4:
            halo = [l4_ref[...], *halo, h4_ref[...]]
        term = t_refs[level][...] + halo_part(level, jnp.concatenate(halo, axis=0))[:n]
        planes = [term[s * PY[level] : (s + 1) * PY[level]] for s in range(EX[level])]
        if total is not None:
            planes = [a + b for a, b in zip(planes, total)]
        fine = level - 1
        wide = dot_left_exact(py[fine][...], jnp.concatenate(planes, axis=1))
        coarse = [wide[:, s * 128 : (s + 1) * 128] for s in range(EX[level])]
        total = []
        for cell in range(LOW[fine], LOW[fine] + EX[fine]):
            value = None
            for k, w in TAPS_AT:
                if (cell - k) % 2 == 0:
                    s = (cell - k) // 2 - LOW[level]
                    if 0 <= s < EX[level]:
                        part = coarse[s] if w == 1.0 else coarse[s] * w
                        value = part if value is None else value + part
            value = masked(value, x_mask(fine, cell)) if fine else value
            total.append(value)
            if fine == 0:
                acc[cell] = value
    halo = jnp.concatenate([lo_ref[pl.ds(0, 8), :], hi_ref[pl.ds(0, 8), :]], axis=0)
    for k in range(4):
        term = halo_part(0, halo[:, k * 512 : (k + 1) * 512])
        for i in range(8):
            s = k * 8 + i
            out_ref[s] = acc[s] + (t_refs[0][pl.ds(s * 64, 64), :] + term[i * 64 : (i + 1) * 64])


VMEM_LIMIT = 24 * 2**20
VM = pl.BlockSpec(memory_space=pltpu.VMEM)
SM = pl.BlockSpec(memory_space=pltpu.SMEM)


def call(body, shapes, in_specs, scratch=(), flops=4 * 10**8):
    return pl.pallas_call(
        body,
        out_shape=[jax.ShapeDtypeStruct(s, d) for s, d in shapes],
        in_specs=in_specs,
        out_specs=[VM] * len(shapes),
        scratch_shapes=list(scratch),
        compiler_params=pltpu.CompilerParams(vmem_limit_bytes=VMEM_LIMIT),
        cost_estimate=pl.CostEstimate(flops=flops, bytes_accessed=2**21, transcendentals=0),
    )


def steps(axis, by):
    count = lax.axis_size(axis)
    return [(i, i + by) for i in range(count) if 0 <= i + by < count]


def per_device(charges, kernel_taps):
    taps = kernel_taps

    def shift(v, axis, by):
        return lax.ppermute(v, axis, steps(axis, by))

    s1f, s1b, s2, v = call(
        restrict_kernel,
        [((1000, 128), F32), ((1000, 128), F32), ((2, 24, 128), F32),
         ((8, 16, 384), F32)],
        [VM], [pltpu.VMEM((13, 24, 128), F32)],
    )(charges)
    l1 = shift(s1f, "gx", 1)
    r1 = shift(s1b, "gx", -1)
    vs = lax.all_to_all(v, "gy", 0, 0)
    near, far = call(coarse_y_kernel, [((48, 128), F32), ((96, 128), F32)], [SM] + [VM] * 2)(taps, vs, s2)
    low = lax.ppermute(near, "gx", [(i, (i + 1) % 4) for i in range(4)])
    high = lax.ppermute(near, "gx", [(i, (i + 3) % 4) for i in range(4)])
    far = lax.ppermute(far, "gx", [(i, (i + 2) % 4) for i in range(4)])
    mats_shapes = [(64, 240), (40, 240), (24, 192)]
    for halo in (16, 32, 32, 32, 64):
        mats_shapes += [(128, 256), (3 * halo, 128)]
    mats_shapes += [(PY[l], 2 * up16(PY[l + 1])) for l in range(4)]
    mats = call(prep_kernel, [(w, BF16) for w in mats_shapes], [SM])(taps)
    my, own, halo, py = mats[:3], mats[3:13:2], mats[4:13:2], mats[13:]
    y0, o, fw, bw, tb = call(
        x_kernel,
        [((32, 64, 128), F32), ((19, 40, 128), F32), ((560, 128), F32), ((560, 128), F32), ((48, 128), F32)],
        [SM] + [VM] * 6,
        [pltpu.VMEM((35, 40, 128), F32), pltpu.VMEM((29, 24, 128), F32)],
    )(taps, charges, s1f, s1b, l1, r1, far)
    lo = shift(fw, "gy", 1)
    hi = shift(bw, "gy", -1)
    z3, z4, t4 = call(
        coarse_kernel, [((144, 128), F32), ((112, 128), F32), ((16, 128), F32)], [VM] * 5,
        [pltpu.VMEM((37, 16, 128), F32), pltpu.VMEM((29, 16, 128), F32)],
    )(tb, near, low, high, far)
    l4 = shift(t4, "gz", 2)
    h4 = shift(t4, "gz", -2)
    z0, z1, z2, fw, bw = call(
        y_kernel, [((Z_ROWS[l], 128), F32) for l in range(3)] + [((24, 2048), F32), ((24, 2048), F32)], [VM] * 9
    )(y0, o, lo, hi, z3, z4, *my[:3])
    z = (z0, z1, z2, z3, z4)
    lo = shift(fw, "gz", 1)
    hi = shift(bw, "gz", -1)
    terms = call(own_kernel, [((Z_ROWS[l], 128), F32) for l in range(5)], [VM] * 10)(*z, *own)
    (out,) = call(
        z_kernel, [((32, 64, 128), F32)], [VM] * 18, [pltpu.VMEM((32, 64, 128), F32)]
    )(*terms, lo, hi, l4, h4, *halo, *py)
    return out


def solution(mesh):
    return jax.shard_map(
        per_device,
        mesh=mesh,
        in_specs=(P("gx", "gy", "gz"), P()),
        out_specs=P("gx", "gy", "gz"),
        check_vma=False,
    )
```

```python
import jax
import jax.numpy as jnp
from jax import lax
from jax.experimental import pallas as pl
from jax.experimental.pallas import tpu as pltpu
from jax.sharding import PartitionSpec as P


F32, BF16, I32 = jnp.float32, jnp.bfloat16, jnp.int32
CUBIC = (-0.0625, 0.0, 0.5625, 1.0, 0.5625, 0.0, -0.0625)
TAPS_AT = tuple((k - 3, w) for k, w in enumerate(CUBIC) if w != 0.0)

DEVICES = (4, 8, 8)
BX, BY, BZ = (32, 16, 8, 4, 2), (64, 32, 16, 8, 4), (128, 64, 32, 16, 8)
LOW = (0, -1, -2, -2, -2)
EX = (32, 19, 13, 9, 7)
EY = (64, 35, 21, 13, 9)
EZ = (128, 67, 37, 21, 13)
PY = (64, 40, 24, 16, 16)
OZ = (0, 0, 67, 104, 44)


def is_even(axis):
    return (lax.axis_index(axis) & 1) == 0


def store_pair(even, a_ref, b_ref, where, up, down):
    a_ref[where] = jnp.where(even, up, down)
    b_ref[where] = jnp.where(even, down, up)


def picked(even, a_ref, b_ref):
    return lambda where: jnp.where(even, a_ref[where], b_ref[where])


FAR = (range(0, 3), range(3, 5))
V_COLUMNS = ((3, range(0, 5)), (3, range(5, 9)), (4, range(0, 7)))


def up16(n):
    return (n + 15) // 16 * 16


def iota(shape, dim):
    return lax.broadcasted_iota(I32, shape, dim)


def in_grid(level, ext, blocks, count, index, position):
    cell = index + LOW[level]
    g = cell + position * blocks[level]
    return (index >= 0) & (index < ext[level]) & (g >= 0) & (g < blocks[level] * count)


def cubic_matrix(level, ext, blocks, count, position, fine, coarse):
    offset = fine + LOW[level] - 2 * (coarse + LOW[level + 1])
    value = jnp.zeros(offset.shape, F32)
    for k, w in TAPS_AT:
        value = jnp.where(offset == k, w, value)
    ok = in_grid(level, ext, blocks, count, fine, position) & in_grid(level + 1, ext, blocks, count, coarse, position)
    return jnp.where(ok, value, 0.0)


def repeated(index, period):
    for _ in range(2):
        index = jnp.where(index >= period, index - period, index)
    return index


def restrict_y(level, position):
    half = up16(PY[level])
    shape = (PY[level + 1], 2 * half)
    return cubic_matrix(level, EY, BY, 8, position, repeated(iota(shape, 1), half), iota(shape, 0)).astype(BF16)


def prolong_y(level, position):
    half = up16(PY[level + 1])
    shape = (PY[level], 2 * half)
    return cubic_matrix(level, EY, BY, 8, position, iota(shape, 0), repeated(iota(shape, 1), half)).astype(BF16)


def restrict_z(level, position):
    shape = (128, 128)
    m = cubic_matrix(level, EZ, BZ, 8, position, iota(shape, 0) - OZ[level], iota(shape, 1) - OZ[level + 1]).astype(BF16)
    return jnp.concatenate([m, m], axis=0)


def split(v):
    hi = v.astype(BF16)
    return hi, (v - hi.astype(F32)).astype(BF16)


def dot(a, b, dims=(((1,), (0,)), ((), ()))):
    return lax.dot_general(a, b, dims, preferred_element_type=F32)


def stacked(value, *order):
    rows = up16(value.shape[0])
    if rows > value.shape[0]:
        value = jnp.concatenate([value, jnp.zeros((rows - value.shape[0], value.shape[1]), F32)], axis=0)
    parts = split(value)
    return jnp.concatenate([parts[k] for k in order], axis=0)


def dot_left_exact(m, b):
    return dot(m, stacked(b, 0, 1))


def dot_right_exact(a, m):
    return dot(jnp.concatenate(split(a), axis=1), m)


def dot3(a, b, dims=(((1,), (0,)), ((), ()))):
    return dot(a[0], b[0], dims) + (dot(a[0], b[1], dims) + dot(a[1], b[0], dims))


def x_mask(level, cell):
    i = lax.axis_index("gx")
    if cell < 0:
        return jnp.where(i * BX[level] + cell >= 0, 1.0, 0.0).astype(F32)
    if cell >= BX[level]:
        return jnp.where(i * BX[level] + cell < BX[level] * DEVICES[0], 1.0, 0.0).astype(F32)
    return None


def masked(value, mask):
    return value if mask is None else value * mask


def lanes_mask(first, count):
    lane = lax.broadcasted_iota(I32, (1, 128), 1)
    return (lane >= first) & (lane < first + count)


def restrict_x(level, slab):
    first, last = LOW[level], LOW[level] + EX[level]
    out = []
    for i in range(LOW[level + 1], LOW[level + 1] + EX[level + 1]):
        total = None
        for k, w in TAPS_AT:
            if first <= 2 * i + k < last:
                term = slab(2 * i + k)
                term = term if w == 1.0 else term * w
                total = term if total is None else total + term
        out.append(masked(total, x_mask(level + 1, i)))
    return out


def restrict_kernel(q_ref, sa_ref, sb_ref, s2_ref, v_ref, far):
    even = is_even("gx")
    for s in range(8):
        store_pair(even, sa_ref, sb_ref, pl.ds(s * 64, 64), q_ref[s + 24], q_ref[s])
    ix, iy, iz = lax.axis_index("gx"), lax.axis_index("gy"), lax.axis_index("gz")
    low = lanes_mask(0, EZ[1])
    slab = lambda i: q_ref[i]
    kept = {}
    for l in range(1, 5):
        planes = restrict_x(l - 1, slab)
        n, rows = EX[l], PY[l]
        wide = jnp.concatenate(planes, axis=1)
        wide = dot_left_exact(restrict_y(l - 1, iy), wide)
        tall = jnp.concatenate([wide[:, s * 128 : (s + 1) * 128] for s in range(n)], axis=0)
        tall = dot_right_exact(tall, restrict_z(l - 1, iz))
        planes = kept[l] = [tall[s * rows : (s + 1) * rows] for s in range(n)]
        slab = lambda i, planes=planes, low=LOW[l]: planes[i - low]
    for s in range(EX[2]):
        far[s] = kept[2][s]
    for s in range(11):
        up, down = kept[1][s + EX[1] - 11], kept[1][s]
        store_pair(even, sa_ref, sb_ref, pl.ds(512 + s * 40, 24), jnp.where(low, up[:24], kept[2][s]), jnp.where(low, down[:24], kept[2][s]))
        store_pair(even, sa_ref, sb_ref, pl.ds(512 + s * 40 + 24, 16), up[24:], down[24:])
    for s in range(11, EX[2]):
        for ref in (sa_ref, sb_ref):
            ref[pl.ds(952 + (s - 11) * 24, 24), :] = kept[2][s]
    start = jnp.where(ix < 2, 8, 0)
    mask = lanes_mask(OZ[2], EZ[2])
    for k, members in enumerate(FAR):
        total = jnp.zeros((24, 128), F32)
        for n, s in enumerate(members):
            total = total + pltpu.roll(jnp.where(mask, far[start + s], 0.0), (n * EZ[2] - OZ[2]) % 128, 1)
        s2_ref[k] = total
    for c, (level, members) in enumerate(V_COLUMNS):
        mask = lanes_mask(OZ[level], EZ[level])
        total = jnp.zeros((16, 128), F32)
        for n, s in enumerate(members):
            value = jnp.where(mask, kept[level][s], 0.0)
            total = total + pltpu.roll(value, (n * EZ[level] - OZ[level]) % 128, 1)
        for d in range(8):
            v_ref[d, :, pl.ds(c * 128, 128)] = total


def conv_x(out_count, taps_ref, level, load, store):
    if len(taps_ref.shape) == 3:
        taps = [taps_ref[level, 0, t] for t in range(17)]
    else:
        taps = [taps_ref[pl.ds((level - 3) * 24 + t, 1), :] for t in range(17)]
    for i in range(out_count):
        total = load(i) * taps[0]
        for t in range(1, 17):
            total = total + load(i + t) * taps[t]
        store(i, total)


def x_kernel(taps_ref, q_ref, sa_ref, sb_ref, ra_ref, rb_ref, f_ref, y0_ref, o_ref, fa_ref, fb_ref, tb_ref, q1, q2):
    ix = lax.axis_index("gx")
    even, even_y = is_even("gx"), is_even("gy")
    below, above = picked(even, rb_ref, ra_ref), picked(even, ra_ref, rb_ref)
    sent_up, sent_down = picked(even, sa_ref, sb_ref), picked(even, sb_ref, sa_ref)
    taps0 = [taps_ref[0, 0, t] for t in range(17)]

    def level0(j, _):
        rows = pl.ds(pl.multiple_of(j * 8, 8), 8)
        for first in (0, 16):
            acc = {}
            for p in range(first, first + 32):
                if p < 8:
                    v = below(pl.ds(pl.multiple_of(p * 64 + j * 8, 8), 8))
                elif p < 40:
                    v = q_ref[p - 8, rows, :]
                else:
                    v = above(pl.ds(pl.multiple_of((p - 40) * 64 + j * 8, 8), 8))
                for t in range(17):
                    i = p - t
                    if first <= i < first + 16:
                        term = v * taps0[t]
                        acc[i] = acc[i] + term if i in acc else term
            for i, value in acc.items():
                y0_ref[i, rows, :] = value
        return 0

    lax.fori_loop(0, 8, level0, 0)
    for i in range(32):
        store_pair(even_y, fa_ref, fb_ref, pl.ds(i * 8, 8), y0_ref[i, pl.ds(56, 8), :], y0_ref[i, pl.ds(0, 8), :])

    def received(ref, at, rows):
        if not 0 <= at < (11 if rows == 40 else 13):
            return None
        return ref(pl.ds(512 + at * 40 if at < 11 else 952 + (at - 11) * 24, rows))

    def added(values):
        values = [v for v in values if v is not None]
        total = values[0]
        for v in values[1:]:
            total = total + v
        return total

    def own(at, rows):
        if rows == 24 or at < 11:
            return received(sent_down, at, rows)
        return received(sent_up, at - 8, rows)

    for r in range(35):
        cell = r - 9
        q1[r] = added([own(cell + 1, 40), received(below, cell + 9, 40), received(above, cell - 15, 40)])
    for r in range(29):
        cell = r - 10
        q2[r] = added([own(cell + 2, 24), received(below, cell + 10, 24), received(above, cell - 6, 24)])
    start = jnp.where(ix < 2, 24, 0)
    mask = lanes_mask(OZ[2], EZ[2])
    for k, members in enumerate(FAR):
        for n, s in enumerate(members):
            q2[start + s] += jnp.where(mask, pltpu.roll(f_ref[k], (OZ[2] - n * EZ[2]) % 128, 1), 0.0)
    low = lanes_mask(0, EZ[1])
    two = {}

    def keep2(i, total):
        two[i] = masked(total, x_mask(2, LOW[2] + i))

    def keep1(s, total):
        total = masked(total, x_mask(1, LOW[1] + s))
        f, b = total[24:40], total[:16]
        o_ref[s, pl.ds(24, 16), :] = f
        o_ref[s, pl.ds(0, 24), :] = jnp.where(low, total[:24], two[s]) if s < EX[2] else total[:24]
        if s < EX[2]:
            f = jnp.where(low, f, two[s][8:])
            b = jnp.where(low, b, two[s][:16])
        store_pair(even_y, fa_ref, fb_ref, pl.ds(256 + s * 16, 16), f, b)

    for level in (3, 4):
        for t in range(17):
            tb_ref[pl.ds((level - 3) * 24 + t, 1), :] = jnp.full((1, 128), taps_ref[level, 0, t], F32)
    conv_x(EX[2], taps_ref, 2, lambda r: q2[r], keep2)
    conv_x(EX[1], taps_ref, 1, lambda r: q1[r], keep1)


def coarse_y_kernel(taps_ref, v_ref, u_ref):
    iy = lax.axis_index("gy")
    block = stacked(jnp.concatenate([v_ref[k] for k in range(8)], axis=0), 0, 1, 0)
    for level, first, last in ((3, 0, 256), (4, 256, 384)):
        i, j = iota((16, 384), 0), iota((16, 384), 1) & 127
        to = out_cells(level, BY, EY, i, iy, 8)
        d, r = j >> 4, j & 15
        at = jnp.where(r < EY[level], (d - iy) * BY[level] + r + LOW[level], BAD)
        out = dot(thirds(toeplitz(taps_ref, level, 1, at - to + 8), 128), block[:, first:last])
        for c in range(first, last, 128):
            u_ref[pl.ds(c // 8, 16), :] = out[:, c - first : c - first + 128]


def coarse_kernel(taps_ref, own_ref, low_ref, high_ref, far_ref, z3_ref, z4_ref, t4_ref, g3, g4):
    ix = lax.axis_index("gx")
    for g in (g3, g4):
        g[...] = jnp.zeros_like(g)
    for ref, step in ((own_ref, 0), (low_ref, 3), (high_ref, 1), (far_ref, 2)):
        source = (ix + step) & 3
        for c, (level, members) in enumerate(V_COLUMNS):
            g = g3 if level == 3 else g4
            column = ref[pl.ds(c * 16, 16), :]
            for n, s in enumerate(members):
                g[source * BX[level] + (LOW[level] + s + 10)] += pltpu.roll(column, (OZ[level] - n * EZ[level]) % 128, 1)
    for level, g, z_ref in ((3, g3, z3_ref), (4, g4, z4_ref)):
        start = ix * BX[level] + 10 + LOW[level] - 8

        def keep(i, total, level=level, z_ref=z_ref):
            z_ref[pl.ds(i * 16, 16), :] = masked(total, x_mask(level, LOW[level] + i))

        conv_x(EX[level], taps_ref, level, lambda r, g=g, start=start: g[start + r], keep)
    t4_ref[...] = level4_rows(z4_ref)


BAD = 1000


def out_cells(level, blocks, ext, index, position, count):
    return jnp.where(in_grid(level, ext, blocks, count, index, position), index + LOW[level], -BAD)


def thirds(value, third):
    hi, lo = split(value)
    return jnp.where(iota(value.shape, 1) < 2 * third, hi.astype(F32), lo.astype(F32)).astype(BF16)


def toeplitz(taps_ref, level, axis, diff):
    total = jnp.zeros(diff.shape, F32)
    for t in range(17):
        total = jnp.where(diff == t, taps_ref[level, axis, t], total)
    return total


def store_z(ref, halo_ref, own, halo):
    ref[...] = jnp.concatenate(split(own), axis=1)
    hi, lo = split(halo)
    halo_ref[...] = jnp.concatenate([hi, hi, lo], axis=0)


def prep_kernel(taps_ref, *out):
    iy = lax.axis_index("gy")
    iz = lax.axis_index("gz")
    outs = out[:3]
    z_outs = [out[3 + 2 * k : 5 + 2 * k] for k in range(5)]

    for level, width, ref in ((0, 80, outs[0]), (1, 80, outs[1]), (2, 64, outs[2])):
        shape = (PY[level], 3 * width)
        i, j = iota(shape, 0), repeated(iota(shape, 1), width)
        to = out_cells(level, BY, EY, i, iy, 8)
        if level == 0:
            at = j - 8
        else:
            halo, reach = 16, 11 if level == 1 else 13
            own = j - halo
            upper = own - PY[level]
            lowest = LOW[level] - 8
            at = jnp.where(
                own < 0,
                jnp.where(j < reach, j + lowest, BAD),
                jnp.where(
                    upper < 0,
                    jnp.where(own < EY[level], own + LOW[level], BAD),
                    jnp.where(upper < reach, upper + LOW[level] + BY[level], BAD),
                ),
            )
        ref[...] = thirds(toeplitz(taps_ref, level, 1, at - to + 8), width)
    j = iota((128, 128), 0)
    c = iota((128, 128), 1)
    own = toeplitz(taps_ref, 0, 2, j - c + 8)
    j, c = iota((16, 128), 0), iota((16, 128), 1)
    store_z(*z_outs[0], own, toeplitz(taps_ref, 0, 2, jnp.where(j < 8, j - 8, j - 8 + 128) - c + 8))
    for level in range(4):
        out[13 + level][...] = prolong_y(level, iy)
    prolong = None
    for level in range(1, 5):
        shape = (128, 128)
        one = cubic_matrix(level - 1, EZ, BZ, 8, iz, iota(shape, 1), iota(shape, 0)).astype(BF16)
        whole = one.astype(F32) if prolong is None else dot(one, prolong[0]) + dot(one, prolong[1])
        prolong = split(whole)
        c = iota((128, 128), 1)
        to = out_cells(level, BZ, EZ, c, iz, 8)
        j = iota((128, 128), 0) - OZ[level]
        at = jnp.where((j >= 0) & (j < EZ[level]), j + LOW[level], BAD)
        own = dot3(split(toeplitz(taps_ref, level, 2, at - to + 8)), prolong)
        rows = 64 if level == 4 else 32
        c = iota((rows, 128), 1)
        to = out_cells(level, BZ, EZ, c, iz, 8)
        j = iota((rows, 128), 0)
        r = j & 15
        if level == 4:
            d = j >> 4
            shift = jnp.where(d == 0, -2, jnp.where(d == 1, -1, jnp.where(d == 2, 1, 2))) * BZ[4]
            at = jnp.where(r < EZ[4], shift + r + LOW[4], BAD)
        else:
            reach = 11 if level == 1 else 13
            at = jnp.where(j < 16, r + LOW[level] - 8, r + LOW[level] + BZ[level])
            at = jnp.where(r < reach, at, BAD)
        store_z(*z_outs[level], own, dot3(split(toeplitz(taps_ref, level, 2, at - to + 8)), prolong))


def level4_rows(z4_ref):
    block = pltpu.roll(z4_ref[...], (-OZ[4]) % 128, 1)
    return jnp.concatenate([block, jnp.zeros((16, 128), F32)], axis=0).T[:16]


def store_rows(even, a_ref, b_ref, at, up, down):
    store_pair(even, a_ref, b_ref, (slice(None), pl.ds(2048 + at, 128)), up[:8], down[:8])
    store_pair(even, a_ref, b_ref, (slice(None), pl.ds(3584 + at, 128)), up[8:], down[8:])


def load_rows(pick, at, count):
    return jnp.concatenate([pick((slice(None), pl.ds(2048 + at, count))), pick((slice(None), pl.ds(3584 + at, count)))], axis=0)


def y_kernel(y0_ref, o_ref, ra_ref, rb_ref, z3_ref, z4_ref, *refs):
    even, even_z = is_even("gy"), is_even("gz")
    below, above = picked(even, rb_ref, ra_ref), picked(even, ra_ref, rb_ref)
    my = [ref[...] for ref in refs[:3]]
    z0_ref, z1_ref, z2_ref, fa_ref, fb_ref = refs[3:]
    for base in range(0, 32, 4):
        parts = []
        for i in range(base, base + 4):
            parts.append(jnp.concatenate(
                [below(pl.ds(i * 8, 8)), y0_ref[i], above(pl.ds(i * 8, 8))], axis=0))
        out = dot(my[0], stacked(jnp.concatenate(parts, axis=1), 0, 1, 0))
        for n in range(4):
            z0_ref[pl.ds((base + n) * 64, 64), :] = out[:, n * 128 : (n + 1) * 128]
    for level, z_ref in ((1, z1_ref), (2, z2_ref)):
        n, rows = EX[level], PY[level]
        parts = [jnp.concatenate([below(pl.ds(256 + s * 16, 16)), o_ref[s, pl.ds(0, rows), :], above(pl.ds(256 + s * 16, 16))], axis=0)
                 for s in range(n)]
        out = dot(my[level], stacked(jnp.concatenate(parts, axis=1), 0, 1, 0))
        for s in range(n):
            z_ref[pl.ds(s * rows, rows), :] = out[:, s * 128 : (s + 1) * 128]
    for k in range(16):
        t = z0_ref[pl.ds(k * 128, 128), :].T
        store_pair(even_z, fa_ref, fb_ref, (slice(None), pl.ds(k * 128, 128)), t[120:], t[:8])
    for k in range(6):
        size = 128 if k < 5 else 120
        block = z1_ref[pl.ds(k * 128, size), :]
        if size < 128:
            block = jnp.concatenate([block, jnp.zeros((128 - size, 128), F32)], axis=0)
        t = block.T
        store_rows(even_z, fa_ref, fb_ref, k * 128, t[56:72], t[0:16])
    for level, z_ref, at, f, count in ((2, z2_ref, 768, 24, 312), (3, z3_ref, 1152, 8, 144)):
        for k in range((count + 127) // 128):
            size = min(128, count - k * 128)
            block = pltpu.roll(z_ref[pl.ds(k * 128, size), :], (-OZ[level]) % 128, 1)
            if size < 128:
                block = jnp.concatenate([block, jnp.zeros((128 - size, 128), F32)], axis=0)
            t = block.T
            store_rows(even_z, fa_ref, fb_ref, at + k * 128, t[f : f + 16], t[0:16])
    t = level4_rows(z4_ref)
    store_rows(even_z, fa_ref, fb_ref, 1408, t, t)


Z_AT = {0: 0, 1: 0, 2: 768, 3: 1152, 4: 1408}
Z_ROWS = {0: 2048, 1: 760, 2: 312, 3: 144, 4: 112}


def own_kernel(*refs):
    for level in range(5):
        z_ref, m_ref, t_ref = refs[level], refs[5 + level], refs[10 + level]
        m = m_ref[...]
        m = jnp.concatenate([m, jnp.concatenate([m[:, :128], jnp.zeros((128, 128), BF16)], axis=1)], axis=0)
        step = 512 if level == 0 else Z_ROWS[level]
        for k in range(0, Z_ROWS[level], step):
            both = dot(jnp.concatenate(split(z_ref[pl.ds(k, step), :]), axis=1), m)
            t_ref[pl.ds(k, step), :] = both[:, :128] + both[:, 128:]


def z_kernel(*refs):
    t_refs, (ra_ref, rb_ref, a4_ref, b4_ref), m_refs, py = refs[:5], refs[5:9], refs[9:14], refs[14:18]
    even, even2 = is_even("gz"), (lax.axis_index("gz") & 2) == 0
    below, above = picked(even, rb_ref, ra_ref), picked(even, ra_ref, rb_ref)
    below2, above2 = picked(even2, b4_ref, a4_ref), picked(even2, a4_ref, b4_ref)
    out_ref, acc = refs[18:]
    first = (((0,), (0,)), ((), ()))

    def halo_part(level, halo):
        return dot(stacked(halo, 0, 1, 0), m_refs[level][...], first)

    total = None
    for level in (4, 3, 2, 1):
        n = Z_ROWS[level]
        halo = [load_rows(ref, Z_AT[level], (n + 127) // 128 * 128) for ref in (below, above)]
        if level == 4:
            halo = [below2(...), *halo, above2(...)]
        term = t_refs[level][...] + halo_part(level, jnp.concatenate(halo, axis=0))[:n]
        planes = [term[s * PY[level] : (s + 1) * PY[level]] for s in range(EX[level])]
        if total is not None:
            planes = [a + b for a, b in zip(planes, total)]
        fine = level - 1
        wide = dot_left_exact(py[fine][...], jnp.concatenate(planes, axis=1))
        coarse = [wide[:, s * 128 : (s + 1) * 128] for s in range(EX[level])]
        total = []
        for cell in range(LOW[fine], LOW[fine] + EX[fine]):
            value = None
            for k, w in TAPS_AT:
                if (cell - k) % 2 == 0:
                    s = (cell - k) // 2 - LOW[level]
                    if 0 <= s < EX[level]:
                        part = coarse[s] if w == 1.0 else coarse[s] * w
                        value = part if value is None else value + part
            value = masked(value, x_mask(fine, cell)) if fine else value
            total.append(value)
            if fine == 0:
                acc[cell] = value
    halo = jnp.concatenate([pick((slice(None), pl.ds(0, 2048))) for pick in (below, above)], axis=0)
    for k in range(4):
        term = halo_part(0, halo[:, k * 512 : (k + 1) * 512])
        for i in range(8):
            s = k * 8 + i
            out_ref[s] = acc[s] + (t_refs[0][pl.ds(s * 64, 64), :] + term[i * 64 : (i + 1) * 64])


VMEM_LIMIT = 24 * 2**20
VM = pl.BlockSpec(memory_space=pltpu.VMEM)
SM = pl.BlockSpec(memory_space=pltpu.SMEM)


def call(body, shapes, in_specs, scratch=(), flops=4 * 10**8):
    return pl.pallas_call(
        body,
        out_shape=[jax.ShapeDtypeStruct(s, d) for s, d in shapes],
        in_specs=in_specs,
        out_specs=[VM] * len(shapes),
        scratch_shapes=list(scratch),
        compiler_params=pltpu.CompilerParams(vmem_limit_bytes=VMEM_LIMIT),
        cost_estimate=pl.CostEstimate(flops=flops, bytes_accessed=2**21, transcendentals=0),
    )


def per_device(charges, kernel_taps):
    taps = kernel_taps

    def swap(v, axis, by=1, second=False):
        count = lax.axis_size(axis)
        partner = lambda i: i ^ by if not second else ((i + by) ^ by) - by
        return lax.ppermute(v, axis, [(i, partner(i)) for i in range(count) if 0 <= partner(i) < count])

    sa, sb, s2, v = call(
        restrict_kernel,
        [((1000, 128), F32), ((1000, 128), F32), ((2, 24, 128), F32),
         ((8, 16, 384), F32)],
        [VM], [pltpu.VMEM((13, 24, 128), F32)],
    )(charges)
    ra = swap(sa, "gx")
    rb = swap(sb, "gx", second=True)
    f2 = lax.ppermute(s2, "gx", [(i, i ^ 2) for i in range(4)])
    vs = lax.all_to_all(v, "gy", 0, 0)
    (u,) = call(coarse_y_kernel, [((48, 128), F32)], [SM, VM])(taps, vs)
    others = []
    for by in (1, 3, 2):
        others.append(lax.ppermute(u, "gx", [(i, (i + by) % 4) for i in range(4)]))
    mats_shapes = [(64, 240), (40, 240), (24, 192)]
    for halo in (16, 32, 32, 32, 64):
        mats_shapes += [(128, 256), (3 * halo, 128)]
    mats_shapes += [(PY[l], 2 * up16(PY[l + 1])) for l in range(4)]
    mats = call(prep_kernel, [(w, BF16) for w in mats_shapes], [SM])(taps)
    my, own, halo, py = mats[:3], mats[3:13:2], mats[4:13:2], mats[13:]
    y0, o, sa, sb, tb = call(
        x_kernel,
        [((32, 64, 128), F32), ((19, 40, 128), F32), ((560, 128), F32), ((560, 128), F32), ((48, 128), F32)],
        [SM] + [VM] * 6,
        [pltpu.VMEM((35, 40, 128), F32), pltpu.VMEM((29, 24, 128), F32)],
    )(taps, charges, sa, sb, ra, rb, f2)
    ra = swap(sa, "gy")
    rb = swap(sb, "gy", second=True)
    z3, z4, t4 = call(
        coarse_kernel, [((144, 128), F32), ((112, 128), F32), ((16, 128), F32)], [VM] * 5,
        [pltpu.VMEM((37, 16, 128), F32), pltpu.VMEM((29, 16, 128), F32)],
    )(tb, u, *others)
    a4 = swap(t4, "gz", 2)
    b4 = swap(t4, "gz", 2, second=True)
    z0, z1, z2, sa, sb = call(
        y_kernel, [((Z_ROWS[l], 128), F32) for l in range(3)] + [((8, 5120), F32), ((8, 5120), F32)], [VM] * 9
    )(y0, o, ra, rb, z3, z4, *my[:3])
    z = (z0, z1, z2, z3, z4)
    ra = swap(sa, "gz")
    rb = swap(sb, "gz", second=True)
    terms = call(own_kernel, [((Z_ROWS[l], 128), F32) for l in range(5)], [VM] * 10)(*z, *own)
    (out,) = call(
        z_kernel, [((32, 64, 128), F32)], [VM] * 18, [pltpu.VMEM((32, 64, 128), F32)]
    )(*terms, ra, rb, a4, b4, *halo, *py)
    return out


def solution(mesh):
    return jax.shard_map(
        per_device,
        mesh=mesh,
        in_specs=(P("gx", "gy", "gz"), P()),
        out_specs=P("gx", "gy", "gz"),
        check_vma=False,
    )
```

```python
import jax
import jax.numpy as jnp
from jax import lax
from jax.experimental import pallas as pl
from jax.experimental.pallas import tpu as pltpu
from jax.sharding import PartitionSpec as P


F32, BF16, I32 = jnp.float32, jnp.bfloat16, jnp.int32
CUBIC = (-0.0625, 0.0, 0.5625, 1.0, 0.5625, 0.0, -0.0625)
TAPS_AT = tuple((k - 3, w) for k, w in enumerate(CUBIC) if w != 0.0)

DEVICES = (4, 8, 8)
BX, BY, BZ = (32, 16, 8, 4, 2), (64, 32, 16, 8, 4), (128, 64, 32, 16, 8)
LOW = (0, -1, -2, -2, -2)
EX = (32, 19, 13, 9, 7)
EY = (64, 35, 21, 13, 9)
EZ = (128, 67, 37, 21, 13)
PY = (64, 40, 24, 16, 16)
OZ = (0, 0, 67, 104, 44)


def is_even(axis):
    return (lax.axis_index(axis) & 1) == 0


def store_pair(even, a_ref, b_ref, where, up, down):
    a_ref[where] = jnp.where(even, up, down)
    b_ref[where] = jnp.where(even, down, up)


def picked(even, a_ref, b_ref):
    return lambda where: jnp.where(even, a_ref[where], b_ref[where])


FAR = (range(0, 3), range(3, 5))
V_COLUMNS = ((3, range(0, 5)), (3, range(5, 9)), (4, range(0, 7)))


def up16(n):
    return (n + 15) // 16 * 16


def iota(shape, dim):
    return lax.broadcasted_iota(I32, shape, dim)


def in_grid(level, ext, blocks, count, index, position):
    cell = index + LOW[level]
    g = cell + position * blocks[level]
    return (index >= 0) & (index < ext[level]) & (g >= 0) & (g < blocks[level] * count)


def cubic_matrix(level, ext, blocks, count, position, fine, coarse):
    offset = fine + LOW[level] - 2 * (coarse + LOW[level + 1])
    value = jnp.zeros(offset.shape, F32)
    for k, w in TAPS_AT:
        value = jnp.where(offset == k, w, value)
    ok = in_grid(level, ext, blocks, count, fine, position) & in_grid(level + 1, ext, blocks, count, coarse, position)
    return jnp.where(ok, value, 0.0)


def repeated(index, period):
    for _ in range(2):
        index = jnp.where(index >= period, index - period, index)
    return index


def restrict_y(level, position):
    half = up16(PY[level])
    shape = (PY[level + 1], 2 * half)
    return cubic_matrix(level, EY, BY, 8, position, repeated(iota(shape, 1), half), iota(shape, 0)).astype(BF16)


def prolong_y(level, position):
    half = up16(PY[level + 1])
    shape = (PY[level], 2 * half)
    return cubic_matrix(level, EY, BY, 8, position, iota(shape, 0), repeated(iota(shape, 1), half)).astype(BF16)


def restrict_z(level, position):
    shape = (128, 128)
    m = cubic_matrix(level, EZ, BZ, 8, position, iota(shape, 0) - OZ[level], iota(shape, 1) - OZ[level + 1]).astype(BF16)
    return jnp.concatenate([m, m], axis=0)


def split(v):
    hi = v.astype(BF16)
    return hi, (v - hi.astype(F32)).astype(BF16)


def dot(a, b, dims=(((1,), (0,)), ((), ()))):
    return lax.dot_general(a, b, dims, preferred_element_type=F32)


def stacked(value, *order):
    rows = up16(value.shape[0])
    if rows > value.shape[0]:
        value = jnp.concatenate([value, jnp.zeros((rows - value.shape[0], value.shape[1]), F32)], axis=0)
    parts = split(value)
    return jnp.concatenate([parts[k] for k in order], axis=0)


def dot_left_exact(m, b):
    return dot(m, stacked(b, 0, 1))


def dot_right_exact(a, m):
    return dot(jnp.concatenate(split(a), axis=1), m)


def dot3(a, b, dims=(((1,), (0,)), ((), ()))):
    return dot(a[0], b[0], dims) + (dot(a[0], b[1], dims) + dot(a[1], b[0], dims))


def x_mask(level, cell):
    i = lax.axis_index("gx")
    if cell < 0:
        return jnp.where(i * BX[level] + cell >= 0, 1.0, 0.0).astype(F32)
    if cell >= BX[level]:
        return jnp.where(i * BX[level] + cell < BX[level] * DEVICES[0], 1.0, 0.0).astype(F32)
    return None


def masked(value, mask):
    return value if mask is None else value * mask


def lanes_mask(first, count):
    lane = lax.broadcasted_iota(I32, (1, 128), 1)
    return (lane >= first) & (lane < first + count)


def restrict_x(level, slab):
    first, last = LOW[level], LOW[level] + EX[level]
    out = []
    for i in range(LOW[level + 1], LOW[level + 1] + EX[level + 1]):
        total = None
        for k, w in TAPS_AT:
            if first <= 2 * i + k < last:
                term = slab(2 * i + k)
                term = term if w == 1.0 else term * w
                total = term if total is None else total + term
        out.append(masked(total, x_mask(level + 1, i)))
    return out


def restrict_kernel(q_ref, sa_ref, sb_ref, s2_ref, v_ref, far):
    even = is_even("gx")
    for s in range(8):
        store_pair(even, sa_ref, sb_ref, pl.ds(s * 64, 64), q_ref[s + 24], q_ref[s])
    ix, iy, iz = lax.axis_index("gx"), lax.axis_index("gy"), lax.axis_index("gz")
    low = lanes_mask(0, EZ[1])
    slab = lambda i: q_ref[i]
    kept = {}
    for l in range(1, 5):
        planes = restrict_x(l - 1, slab)
        n, rows = EX[l], PY[l]
        wide = jnp.concatenate(planes, axis=1)
        wide = dot_left_exact(restrict_y(l - 1, iy), wide)
        tall = jnp.concatenate([wide[:, s * 128 : (s + 1) * 128] for s in range(n)], axis=0)
        tall = dot_right_exact(tall, restrict_z(l - 1, iz))
        planes = kept[l] = [tall[s * rows : (s + 1) * rows] for s in range(n)]
        slab = lambda i, planes=planes, low=LOW[l]: planes[i - low]
    for s in range(EX[2]):
        far[s] = kept[2][s]
    for s in range(11):
        up, down = kept[1][s + EX[1] - 11], kept[1][s]
        store_pair(even, sa_ref, sb_ref, pl.ds(512 + s * 40, 24), jnp.where(low, up[:24], kept[2][s]), jnp.where(low, down[:24], kept[2][s]))
        up, down = up[24:], down[24:]
        if s < 6:
            k, at = divmod(s, 3)
            extra = jnp.concatenate([kept[2][11 + k][at * 8 : at * 8 + 8], jnp.zeros((8, 128), F32)], axis=0)
            up, down = jnp.where(low, up, extra), jnp.where(low, down, extra)
        store_pair(even, sa_ref, sb_ref, pl.ds(512 + s * 40 + 24, 16), up, down)
    start = jnp.where(ix < 2, 8, 0)
    mask = lanes_mask(OZ[2], EZ[2])
    for k, members in enumerate(FAR):
        total = jnp.zeros((24, 128), F32)
        for n, s in enumerate(members):
            total = total + pltpu.roll(jnp.where(mask, far[start + s], 0.0), (n * EZ[2] - OZ[2]) % 128, 1)
        s2_ref[k] = total
    for c, (level, members) in enumerate(V_COLUMNS):
        mask = lanes_mask(OZ[level], EZ[level])
        total = jnp.zeros((16, 128), F32)
        for n, s in enumerate(members):
            value = jnp.where(mask, kept[level][s], 0.0)
            total = total + pltpu.roll(value, (n * EZ[level] - OZ[level]) % 128, 1)
        for d in range(8):
            v_ref[d, :, pl.ds(c * 128, 128)] = total


def conv_x(out_count, taps_ref, level, load, store):
    if len(taps_ref.shape) == 3:
        taps = [taps_ref[level, 0, t] for t in range(17)]
    else:
        taps = [taps_ref[pl.ds((level - 3) * 24 + t, 1), :] for t in range(17)]
    for i in range(out_count):
        total = load(i) * taps[0]
        for t in range(1, 17):
            total = total + load(i + t) * taps[t]
        store(i, total)


def x_kernel(taps_ref, q_ref, sa_ref, sb_ref, ra_ref, rb_ref, f_ref, y0_ref, o_ref, fa_ref, fb_ref, tb_ref, q1, q2):
    ix = lax.axis_index("gx")
    even, even_y = is_even("gx"), is_even("gy")
    below, above = picked(even, rb_ref, ra_ref), picked(even, ra_ref, rb_ref)
    sent_up, sent_down = picked(even, sa_ref, sb_ref), picked(even, sb_ref, sa_ref)
    taps0 = [taps_ref[0, 0, t] for t in range(17)]

    def level0(j, _):
        rows = pl.ds(pl.multiple_of(j * 8, 8), 8)
        for first in (0, 16):
            acc = {}
            for p in range(first, first + 32):
                if p < 8:
                    v = below(pl.ds(pl.multiple_of(p * 64 + j * 8, 8), 8))
                elif p < 40:
                    v = q_ref[p - 8, rows, :]
                else:
                    v = above(pl.ds(pl.multiple_of((p - 40) * 64 + j * 8, 8), 8))
                for t in range(17):
                    i = p - t
                    if first <= i < first + 16:
                        term = v * taps0[t]
                        acc[i] = acc[i] + term if i in acc else term
            for i, value in acc.items():
                y0_ref[i, rows, :] = value
        return 0

    lax.fori_loop(0, 8, level0, 0)
    for i in range(32):
        store_pair(even_y, fa_ref, fb_ref, pl.ds(i * 8, 8), y0_ref[i, pl.ds(56, 8), :], y0_ref[i, pl.ds(0, 8), :])

    def received(ref, at, rows):
        if not 0 <= at < (11 if rows == 40 else 13):
            return None
        if at < 11:
            return ref(pl.ds(512 + at * 40, rows))
        return jnp.concatenate([ref(pl.ds(512 + ((at - 11) * 3 + k) * 40 + 24, 8)) for k in range(3)], axis=0)

    def added(values):
        values = [v for v in values if v is not None]
        total = values[0]
        for v in values[1:]:
            total = total + v
        return total

    def own(at, rows):
        if rows == 24 or at < 11:
            return received(sent_down, at, rows)
        return received(sent_up, at - 8, rows)

    for r in range(35):
        cell = r - 9
        q1[r] = added([own(cell + 1, 40), received(below, cell + 9, 40), received(above, cell - 15, 40)])
    for r in range(29):
        cell = r - 10
        q2[r] = added([own(cell + 2, 24), received(below, cell + 10, 24), received(above, cell - 6, 24)])
    start = jnp.where(ix < 2, 24, 0)
    mask = lanes_mask(OZ[2], EZ[2])
    for k, members in enumerate(FAR):
        for n, s in enumerate(members):
            q2[start + s] += jnp.where(mask, pltpu.roll(f_ref[k], (OZ[2] - n * EZ[2]) % 128, 1), 0.0)
    low = lanes_mask(0, EZ[1])
    two = {}

    def keep2(i, total):
        two[i] = masked(total, x_mask(2, LOW[2] + i))

    def keep1(s, total):
        total = masked(total, x_mask(1, LOW[1] + s))
        f, b = total[24:40], total[:16]
        o_ref[s, pl.ds(24, 16), :] = f
        o_ref[s, pl.ds(0, 24), :] = jnp.where(low, total[:24], two[s]) if s < EX[2] else total[:24]
        if s < EX[2]:
            f = jnp.where(low, f, two[s][8:])
            b = jnp.where(low, b, two[s][:16])
        store_pair(even_y, fa_ref, fb_ref, pl.ds(256 + s * 16, 16), f, b)

    for level in (3, 4):
        for t in range(17):
            tb_ref[pl.ds((level - 3) * 24 + t, 1), :] = jnp.full((1, 128), taps_ref[level, 0, t], F32)
    conv_x(EX[2], taps_ref, 2, lambda r: q2[r], keep2)
    conv_x(EX[1], taps_ref, 1, lambda r: q1[r], keep1)


def coarse_y_kernel(taps_ref, v_ref, u_ref, *outs):
    iy = lax.axis_index("gy")
    block = stacked(jnp.concatenate([v_ref[k] for k in range(8)], axis=0), 0, 1, 0)
    for level, first, last in ((3, 0, 256), (4, 256, 384)):
        i, j = iota((16, 384), 0), iota((16, 384), 1) & 127
        to = out_cells(level, BY, EY, i, iy, 8)
        d, r = j >> 4, j & 15
        at = jnp.where(r < EY[level], (d - iy) * BY[level] + r + LOW[level], BAD)
        out = dot(thirds(toeplitz(taps_ref, level, 1, at - to + 8), 128), block[:, first:last])
        for c in range(first, last, 128):
            u_ref[pl.ds(c // 8, 16), :] = out[:, c - first : c - first + 128]
    for level, width, ref in ((0, 80, outs[0]), (1, 80, outs[1]), (2, 64, outs[2])):
        shape = (PY[level], 3 * width)
        i, j = iota(shape, 0), repeated(iota(shape, 1), width)
        to = out_cells(level, BY, EY, i, iy, 8)
        if level == 0:
            at = j - 8
        else:
            halo, reach = 16, 11 if level == 1 else 13
            own = j - halo
            upper = own - PY[level]
            lowest = LOW[level] - 8
            at = jnp.where(
                own < 0,
                jnp.where(j < reach, j + lowest, BAD),
                jnp.where(
                    upper < 0,
                    jnp.where(own < EY[level], own + LOW[level], BAD),
                    jnp.where(upper < reach, upper + LOW[level] + BY[level], BAD),
                ),
            )
        ref[...] = thirds(toeplitz(taps_ref, level, 1, at - to + 8), width)


def coarse_kernel(taps_ref, own_ref, r1_ref, r2_ref, r3_ref, z3_ref, z4_ref, t4_ref, g3, g4):
    ix = lax.axis_index("gx")
    for g in (g3, g4):
        g[...] = jnp.zeros_like(g)
    for ref, step in ((own_ref, 0), (r1_ref, 1), (r2_ref, 2), (r3_ref, 3)):
        source = ix ^ step
        for c, (level, members) in enumerate(V_COLUMNS):
            g = g3 if level == 3 else g4
            column = ref[pl.ds(c * 16, 16), :]
            for n, s in enumerate(members):
                g[source * BX[level] + (LOW[level] + s + 10)] += pltpu.roll(column, (OZ[level] - n * EZ[level]) % 128, 1)
    for level, g, z_ref in ((3, g3, z3_ref), (4, g4, z4_ref)):
        start = ix * BX[level] + 10 + LOW[level] - 8

        def keep(i, total, level=level, z_ref=z_ref):
            z_ref[pl.ds(i * 16, 16), :] = masked(total, x_mask(level, LOW[level] + i))

        conv_x(EX[level], taps_ref, level, lambda r, g=g, start=start: g[start + r], keep)
    t4_ref[...] = level4_rows(z4_ref)


BAD = 1000


def out_cells(level, blocks, ext, index, position, count):
    return jnp.where(in_grid(level, ext, blocks, count, index, position), index + LOW[level], -BAD)


def thirds(value, third):
    hi, lo = split(value)
    return jnp.where(iota(value.shape, 1) < 2 * third, hi.astype(F32), lo.astype(F32)).astype(BF16)


def toeplitz(taps_ref, level, axis, diff):
    total = jnp.zeros(diff.shape, F32)
    for t in range(17):
        total = jnp.where(diff == t, taps_ref[level, axis, t], total)
    return total


def store_z(ref, halo_ref, own, halo):
    ref[...] = jnp.concatenate(split(own), axis=1)
    hi, lo = split(halo)
    halo_ref[...] = jnp.concatenate([hi, hi, lo], axis=0)


def prep_z_kernel(taps_ref, *out):
    iy = lax.axis_index("gy")
    iz = lax.axis_index("gz")
    z_outs = [out[2 * k : 2 * k + 2] for k in range(5)]
    j = iota((128, 128), 0)
    c = iota((128, 128), 1)
    own = toeplitz(taps_ref, 0, 2, j - c + 8)
    j, c = iota((16, 128), 0), iota((16, 128), 1)
    store_z(*z_outs[0], own, toeplitz(taps_ref, 0, 2, jnp.where(j < 8, j - 8, j - 8 + 128) - c + 8))
    for level in range(4):
        out[10 + level][...] = prolong_y(level, iy)
    prolong = None
    for level in range(1, 5):
        shape = (128, 128)
        one = cubic_matrix(level - 1, EZ, BZ, 8, iz, iota(shape, 1), iota(shape, 0)).astype(BF16)
        whole = one.astype(F32) if prolong is None else dot(one, prolong[0]) + dot(one, prolong[1])
        prolong = split(whole)
        c = iota((128, 128), 1)
        to = out_cells(level, BZ, EZ, c, iz, 8)
        j = iota((128, 128), 0) - OZ[level]
        at = jnp.where((j >= 0) & (j < EZ[level]), j + LOW[level], BAD)
        own = dot3(split(toeplitz(taps_ref, level, 2, at - to + 8)), prolong)
        rows = 64 if level == 4 else 32
        c = iota((rows, 128), 1)
        to = out_cells(level, BZ, EZ, c, iz, 8)
        j = iota((rows, 128), 0)
        r = j & 15
        if level == 4:
            d = j >> 4
            shift = jnp.where(d == 0, -2, jnp.where(d == 1, -1, jnp.where(d == 2, 1, 2))) * BZ[4]
            at = jnp.where(r < EZ[4], shift + r + LOW[4], BAD)
        else:
            reach = 11 if level == 1 else 13
            at = jnp.where(j < 16, r + LOW[level] - 8, r + LOW[level] + BZ[level])
            at = jnp.where(r < reach, at, BAD)
        store_z(*z_outs[level], own, dot3(split(toeplitz(taps_ref, level, 2, at - to + 8)), prolong))


def level4_rows(z4_ref):
    block = pltpu.roll(z4_ref[...], (-OZ[4]) % 128, 1)
    return jnp.concatenate([block, jnp.zeros((16, 128), F32)], axis=0).T[:16]


def store_rows(even, a_ref, b_ref, at, up, down):
    store_pair(even, a_ref, b_ref, (slice(None), pl.ds(2048 + at, 128)), up[:8], down[:8])
    if at == 1408:
        store_pair(even, a_ref, b_ref, (slice(None), pl.ds(4352, 128)), up[8:], down[8:])


def store_rest(even, a_ref, b_ref, at, first, second):
    row = iota((8, 128), 0)
    up, down = [jnp.where(row < 3, f[8:], pltpu.roll(s[8:], 3, 0)) for f, s in zip(first, second)]
    store_pair(even, a_ref, b_ref, (slice(None), pl.ds(3584 + at, 128)), up, down)


def load_rows(pick, level, at, count):
    start = {1: 3584, 2: 3584, 3: 3968, 4: 4352}[level]
    rest = pick((slice(None), pl.ds(start, count)))
    if level in (2, 3):
        rest = pltpu.roll(rest, 5, 0)
    return jnp.concatenate([pick((slice(None), pl.ds(2048 + at, count))), rest], axis=0)


def y_kernel(y0_ref, o_ref, ra_ref, rb_ref, z3_ref, z4_ref, *refs):
    even, even_z = is_even("gy"), is_even("gz")
    below, above = picked(even, rb_ref, ra_ref), picked(even, ra_ref, rb_ref)
    my = [ref[...] for ref in refs[:3]]
    z0_ref, z1_ref, z2_ref, fa_ref, fb_ref = refs[3:]
    for base in range(0, 32, 4):
        parts = []
        for i in range(base, base + 4):
            parts.append(jnp.concatenate(
                [below(pl.ds(i * 8, 8)), y0_ref[i], above(pl.ds(i * 8, 8))], axis=0))
        out = dot(my[0], stacked(jnp.concatenate(parts, axis=1), 0, 1, 0))
        for n in range(4):
            z0_ref[pl.ds((base + n) * 64, 64), :] = out[:, n * 128 : (n + 1) * 128]
    for level, z_ref in ((1, z1_ref), (2, z2_ref)):
        n, rows = EX[level], PY[level]
        parts = [jnp.concatenate([below(pl.ds(256 + s * 16, 16)), o_ref[s, pl.ds(0, rows), :], above(pl.ds(256 + s * 16, 16))], axis=0)
                 for s in range(n)]
        out = dot(my[level], stacked(jnp.concatenate(parts, axis=1), 0, 1, 0))
        for s in range(n):
            z_ref[pl.ds(s * rows, rows), :] = out[:, s * 128 : (s + 1) * 128]
    for k in range(16):
        t = z0_ref[pl.ds(k * 128, 128), :].T
        store_pair(even_z, fa_ref, fb_ref, (slice(None), pl.ds(k * 128, 128)), t[120:], t[:8])
    firsts, seconds = [], []
    for k in range(6):
        size = 128 if k < 5 else 120
        block = z1_ref[pl.ds(k * 128, size), :]
        if size < 128:
            block = jnp.concatenate([block, jnp.zeros((128 - size, 128), F32)], axis=0)
        t = block.T
        store_rows(even_z, fa_ref, fb_ref, k * 128, t[56:72], t[0:16])
        firsts.append((t[56:72], t[0:16]))
    for level, z_ref, at, f, count in ((2, z2_ref, 768, 24, 312), (3, z3_ref, 1152, 8, 144)):
        for k in range((count + 127) // 128):
            size = min(128, count - k * 128)
            block = pltpu.roll(z_ref[pl.ds(k * 128, size), :], (-OZ[level]) % 128, 1)
            if size < 128:
                block = jnp.concatenate([block, jnp.zeros((128 - size, 128), F32)], axis=0)
            t = block.T
            store_rows(even_z, fa_ref, fb_ref, at + k * 128, t[f : f + 16], t[0:16])
            seconds.append((t[f : f + 16], t[0:16]))
    seconds.append(seconds[-1])
    for k in range(6):
        store_rest(even_z, fa_ref, fb_ref, k * 128, firsts[k], seconds[k])
    t = level4_rows(z4_ref)
    store_rows(even_z, fa_ref, fb_ref, 1408, t, t)


Z_AT = {0: 0, 1: 0, 2: 768, 3: 1152, 4: 1408}
Z_ROWS = {0: 2048, 1: 760, 2: 312, 3: 144, 4: 112}


def own_kernel(*refs):
    for level in range(5):
        z_ref, m_ref, t_ref = refs[level], refs[5 + level], refs[10 + level]
        m = m_ref[...]
        m = jnp.concatenate([m, jnp.concatenate([m[:, :128], jnp.zeros((128, 128), BF16)], axis=1)], axis=0)
        step = 512 if level == 0 else Z_ROWS[level]
        for k in range(0, Z_ROWS[level], step):
            both = dot(jnp.concatenate(split(z_ref[pl.ds(k, step), :]), axis=1), m)
            t_ref[pl.ds(k, step), :] = both[:, :128] + both[:, 128:]


def z_kernel(*refs):
    t_refs, (ra_ref, rb_ref, a4_ref, b4_ref), m_refs, py = refs[:5], refs[5:9], refs[9:14], refs[14:18]
    even, even2 = is_even("gz"), (lax.axis_index("gz") & 2) == 0
    below, above = picked(even, rb_ref, ra_ref), picked(even, ra_ref, rb_ref)
    below2, above2 = picked(even2, b4_ref, a4_ref), picked(even2, a4_ref, b4_ref)
    out_ref, acc = refs[18:]
    first = (((0,), (0,)), ((), ()))

    def halo_part(level, halo):
        return dot(stacked(halo, 0, 1, 0), m_refs[level][...], first)

    total = None
    for level in (4, 3, 2, 1):
        n = Z_ROWS[level]
        halo = [load_rows(ref, level, Z_AT[level], (n + 127) // 128 * 128) for ref in (below, above)]
        if level == 4:
            halo = [below2(...), *halo, above2(...)]
        term = t_refs[level][...] + halo_part(level, jnp.concatenate(halo, axis=0))[:n]
        planes = [term[s * PY[level] : (s + 1) * PY[level]] for s in range(EX[level])]
        if total is not None:
            planes = [a + b for a, b in zip(planes, total)]
        fine = level - 1
        wide = dot_left_exact(py[fine][...], jnp.concatenate(planes, axis=1))
        coarse = [wide[:, s * 128 : (s + 1) * 128] for s in range(EX[level])]
        total = []
        for cell in range(LOW[fine], LOW[fine] + EX[fine]):
            value = None
            for k, w in TAPS_AT:
                if (cell - k) % 2 == 0:
                    s = (cell - k) // 2 - LOW[level]
                    if 0 <= s < EX[level]:
                        part = coarse[s] if w == 1.0 else coarse[s] * w
                        value = part if value is None else value + part
            value = masked(value, x_mask(fine, cell)) if fine else value
            total.append(value)
            if fine == 0:
                acc[cell] = value
    halo = jnp.concatenate([pick((slice(None), pl.ds(0, 2048))) for pick in (below, above)], axis=0)
    for k in range(4):
        term = halo_part(0, halo[:, k * 512 : (k + 1) * 512])
        for i in range(8):
            s = k * 8 + i
            out_ref[s] = acc[s] + (t_refs[0][pl.ds(s * 64, 64), :] + term[i * 64 : (i + 1) * 64])


VMEM_LIMIT = 24 * 2**20
VM = pl.BlockSpec(memory_space=pltpu.VMEM)
SM = pl.BlockSpec(memory_space=pltpu.SMEM)


def call(body, shapes, in_specs, scratch=(), flops=4 * 10**8):
    return pl.pallas_call(
        body,
        out_shape=[jax.ShapeDtypeStruct(s, d) for s, d in shapes],
        in_specs=in_specs,
        out_specs=[VM] * len(shapes),
        scratch_shapes=list(scratch),
        compiler_params=pltpu.CompilerParams(vmem_limit_bytes=VMEM_LIMIT),
        cost_estimate=pl.CostEstimate(flops=flops, bytes_accessed=2**21, transcendentals=0),
    )


def prepared(body, shapes, taps):
    return call(body, [(w, BF16) for w in shapes], [SM])(taps)


def per_device(charges, kernel_taps):
    taps = kernel_taps

    def swap(v, axis, by=1, second=False):
        count = lax.axis_size(axis)
        partner = lambda i: i ^ by if not second else ((i + by) ^ by) - by
        return lax.ppermute(v, axis, [(i, partner(i)) for i in range(count) if 0 <= partner(i) < count])

    sa, sb, s2, v = call(
        restrict_kernel,
        [((952, 128), F32), ((952, 128), F32), ((2, 24, 128), F32),
         ((8, 16, 384), F32)],
        [VM], [pltpu.VMEM((13, 24, 128), F32)],
    )(charges)
    ra = swap(sa, "gx")
    rb = swap(sb, "gx", second=True)
    f2 = lax.ppermute(s2, "gx", [(i, i ^ 2) for i in range(4)])
    vs = lax.all_to_all(v, "gy", 0, 0)
    u, *my = call(
        coarse_y_kernel, [((48, 128), F32), ((64, 240), BF16), ((40, 240), BF16), ((24, 192), BF16)], [SM, VM]
    )(taps, vs)
    others = []
    for by in (1, 2, 3):
        others.append(lax.ppermute(u, "gx", [(i, i ^ by) for i in range(4)]))
    z_shapes = []
    for halo in (16, 32, 32, 32, 64):
        z_shapes += [(128, 256), (3 * halo, 128)]
    z_shapes += [(PY[l], 2 * up16(PY[l + 1])) for l in range(4)]
    mats = prepared(prep_z_kernel, z_shapes, taps)
    own, halo, py = mats[:10:2], mats[1:10:2], mats[10:]
    y0, o, sa, sb, tb = call(
        x_kernel,
        [((32, 64, 128), F32), ((19, 40, 128), F32), ((560, 128), F32), ((560, 128), F32), ((48, 128), F32)],
        [SM] + [VM] * 6,
        [pltpu.VMEM((35, 40, 128), F32), pltpu.VMEM((29, 24, 128), F32)],
    )(taps, charges, sa, sb, ra, rb, f2)
    ra = swap(sa, "gy")
    rb = swap(sb, "gy", second=True)
    z3, z4, t4 = call(
        coarse_kernel, [((144, 128), F32), ((112, 128), F32), ((16, 128), F32)], [VM] * 5,
        [pltpu.VMEM((37, 16, 128), F32), pltpu.VMEM((29, 16, 128), F32)],
    )(tb, u, *others)
    a4 = swap(t4, "gz", 2)
    b4 = swap(t4, "gz", 2, second=True)
    z0, z1, z2, sa, sb = call(
        y_kernel, [((Z_ROWS[l], 128), F32) for l in range(3)] + [((8, 4480), F32), ((8, 4480), F32)], [VM] * 9
    )(y0, o, ra, rb, z3, z4, *my)
    z = (z0, z1, z2, z3, z4)
    ra = swap(sa, "gz")
    rb = swap(sb, "gz", second=True)
    terms = call(own_kernel, [((Z_ROWS[l], 128), F32) for l in range(5)], [VM] * 10)(*z, *own)
    (out,) = call(
        z_kernel, [((32, 64, 128), F32)], [VM] * 18, [pltpu.VMEM((32, 64, 128), F32)]
    )(*terms, ra, rb, a4, b4, *halo, *py)
    return out


def solution(mesh):
    return jax.shard_map(
        per_device,
        mesh=mesh,
        in_specs=(P("gx", "gy", "gz"), P()),
        out_specs=P("gx", "gy", "gz"),
        check_vma=False,
    )
```

```python
import jax
import jax.numpy as jnp
from jax import lax
from jax.experimental import pallas as pl
from jax.experimental.pallas import tpu as pltpu
from jax.sharding import PartitionSpec as P


F32, BF16, I32 = jnp.float32, jnp.bfloat16, jnp.int32
CUBIC = (-0.0625, 0.0, 0.5625, 1.0, 0.5625, 0.0, -0.0625)
TAPS_AT = tuple((k - 3, w) for k, w in enumerate(CUBIC) if w != 0.0)

DEVICES = (4, 8, 8)
BX, BY, BZ = (32, 16, 8, 4, 2), (64, 32, 16, 8, 4), (128, 64, 32, 16, 8)
LOW = (0, -1, -2, -2, -2)
EX = (32, 19, 13, 9, 7)
EY = (64, 35, 21, 13, 9)
EZ = (128, 67, 37, 21, 13)
PY = (64, 40, 24, 16, 16)
OZ = (0, 0, 67, 104, 44)


def is_even(axis):
    return (lax.axis_index(axis) & 1) == 0


def store_pair(even, a_ref, b_ref, where, up, down):
    a_ref[where] = jnp.where(even, up, down)
    b_ref[where] = jnp.where(even, down, up)


def picked(even, a_ref, b_ref):
    return lambda where: jnp.where(even, a_ref[where], b_ref[where])


FAR = (range(0, 3), range(3, 5))
V_COLUMNS = ((3, range(0, 5)), (3, range(5, 9)), (4, range(0, 7)))


def up16(n):
    return (n + 15) // 16 * 16


def iota(shape, dim):
    return lax.broadcasted_iota(I32, shape, dim)


def in_grid(level, ext, blocks, count, index, position):
    cell = index + LOW[level]
    g = cell + position * blocks[level]
    return (index >= 0) & (index < ext[level]) & (g >= 0) & (g < blocks[level] * count)


def cubic_matrix(level, ext, blocks, count, position, fine, coarse):
    offset = fine + LOW[level] - 2 * (coarse + LOW[level + 1])
    value = jnp.zeros(offset.shape, F32)
    for k, w in TAPS_AT:
        value = jnp.where(offset == k, w, value)
    ok = in_grid(level, ext, blocks, count, fine, position) & in_grid(level + 1, ext, blocks, count, coarse, position)
    return jnp.where(ok, value, 0.0)


def repeated(index, period):
    for _ in range(2):
        index = jnp.where(index >= period, index - period, index)
    return index


def restrict_y(level, position):
    half = up16(PY[level])
    shape = (PY[level + 1], 2 * half)
    return cubic_matrix(level, EY, BY, 8, position, repeated(iota(shape, 1), half), iota(shape, 0)).astype(BF16)


def prolong_y(level, position):
    half = up16(PY[level + 1])
    shape = (PY[level], 2 * half)
    return cubic_matrix(level, EY, BY, 8, position, iota(shape, 0), repeated(iota(shape, 1), half)).astype(BF16)


def restrict_z(level, position):
    shape = (128, 128)
    m = cubic_matrix(level, EZ, BZ, 8, position, iota(shape, 0) - OZ[level], iota(shape, 1) - OZ[level + 1]).astype(BF16)
    return jnp.concatenate([m, m], axis=0)


def split(v):
    hi = v.astype(BF16)
    return hi, (v - hi.astype(F32)).astype(BF16)


def dot(a, b, dims=(((1,), (0,)), ((), ()))):
    return lax.dot_general(a, b, dims, preferred_element_type=F32)


def stacked(value, *order):
    rows = up16(value.shape[0])
    if rows > value.shape[0]:
        value = jnp.concatenate([value, jnp.zeros((rows - value.shape[0], value.shape[1]), F32)], axis=0)
    parts = split(value)
    return jnp.concatenate([parts[k] for k in order], axis=0)


def dot_left_exact(m, b):
    return dot(m, stacked(b, 0, 1))


def dot_right_exact(a, m):
    return dot(jnp.concatenate(split(a), axis=1), m)


def dot3(a, b, dims=(((1,), (0,)), ((), ()))):
    return dot(a[0], b[0], dims) + (dot(a[0], b[1], dims) + dot(a[1], b[0], dims))


def x_mask(level, cell):
    i = lax.axis_index("gx")
    if cell < 0:
        return jnp.where(i * BX[level] + cell >= 0, 1.0, 0.0).astype(F32)
    if cell >= BX[level]:
        return jnp.where(i * BX[level] + cell < BX[level] * DEVICES[0], 1.0, 0.0).astype(F32)
    return None


def masked(value, mask):
    return value if mask is None else value * mask


def lanes_mask(first, count):
    lane = lax.broadcasted_iota(I32, (1, 128), 1)
    return (lane >= first) & (lane < first + count)


def restrict_x(level, slab):
    first, last = LOW[level], LOW[level] + EX[level]
    out = []
    for i in range(LOW[level + 1], LOW[level + 1] + EX[level + 1]):
        total = None
        for k, w in TAPS_AT:
            if first <= 2 * i + k < last:
                term = slab(2 * i + k)
                term = term if w == 1.0 else term * w
                total = term if total is None else total + term
        out.append(masked(total, x_mask(level + 1, i)))
    return out


def restrict_kernel(q_ref, sa_ref, sb_ref, s2_ref, v_ref, far):
    even = is_even("gx")
    for s in range(8):
        store_pair(even, sa_ref, sb_ref, pl.ds(s * 64, 64), q_ref[s + 24], q_ref[s])
    ix, iy, iz = lax.axis_index("gx"), lax.axis_index("gy"), lax.axis_index("gz")
    low = lanes_mask(0, EZ[1])
    slab = lambda i: q_ref[i]
    kept = {}
    for l in range(1, 5):
        planes = restrict_x(l - 1, slab)
        n, rows = EX[l], PY[l]
        wide = jnp.concatenate(planes, axis=1)
        wide = dot_left_exact(restrict_y(l - 1, iy), wide)
        tall = jnp.concatenate([wide[:, s * 128 : (s + 1) * 128] for s in range(n)], axis=0)
        tall = dot_right_exact(tall, restrict_z(l - 1, iz))
        planes = kept[l] = [tall[s * rows : (s + 1) * rows] for s in range(n)]
        slab = lambda i, planes=planes, low=LOW[l]: planes[i - low]
    for s in range(EX[2]):
        far[s] = kept[2][s]
    for s in range(11):
        up, down = kept[1][s + EX[1] - 11], kept[1][s]
        store_pair(even, sa_ref, sb_ref, pl.ds(512 + s * 40, 24), jnp.where(low, up[:24], kept[2][s]), jnp.where(low, down[:24], kept[2][s]))
        up, down = up[24:], down[24:]
        if s < 6:
            k, at = divmod(s, 3)
            extra = jnp.concatenate([kept[2][11 + k][at * 8 : at * 8 + 8], jnp.zeros((8, 128), F32)], axis=0)
            up, down = jnp.where(low, up, extra), jnp.where(low, down, extra)
        store_pair(even, sa_ref, sb_ref, pl.ds(512 + s * 40 + 24, 16), up, down)
    start = jnp.where(ix < 2, 8, 0)
    mask = lanes_mask(OZ[2], EZ[2])
    for k, members in enumerate(FAR):
        total = jnp.zeros((24, 128), F32)
        for n, s in enumerate(members):
            total = total + pltpu.roll(jnp.where(mask, far[start + s], 0.0), (n * EZ[2] - OZ[2]) % 128, 1)
        s2_ref[k] = total
    for c, (level, members) in enumerate(V_COLUMNS):
        mask = lanes_mask(OZ[level], EZ[level])
        total = jnp.zeros((16, 128), F32)
        for n, s in enumerate(members):
            value = jnp.where(mask, kept[level][s], 0.0)
            total = total + pltpu.roll(value, (n * EZ[level] - OZ[level]) % 128, 1)
        for d in range(8):
            v_ref[d, :, pl.ds(c * 128, 128)] = total


def conv_x(out_count, taps_ref, level, load, store):
    if len(taps_ref.shape) == 3:
        taps = [taps_ref[level, 0, t] for t in range(17)]
    else:
        taps = [taps_ref[pl.ds((level - 3) * 24 + t, 1), :] for t in range(17)]
    for i in range(out_count):
        total = load(i) * taps[0]
        for t in range(1, 17):
            total = total + load(i + t) * taps[t]
        store(i, total)


def x_kernel(taps_ref, q_ref, sa_ref, sb_ref, ra_ref, rb_ref, f_ref, y0_ref, o_ref, fa_ref, fb_ref, tb_ref, q1, q2):
    ix = lax.axis_index("gx")
    even, even_y = is_even("gx"), is_even("gy")
    below, above = picked(even, rb_ref, ra_ref), picked(even, ra_ref, rb_ref)
    sent_up, sent_down = picked(even, sa_ref, sb_ref), picked(even, sb_ref, sa_ref)
    taps0 = [taps_ref[0, 0, t] for t in range(17)]

    def level0(j, _):
        rows = pl.ds(pl.multiple_of(j * 8, 8), 8)
        for first in (0, 16):
            acc = {}
            for p in range(first, first + 32):
                if p < 8:
                    v = below(pl.ds(pl.multiple_of(p * 64 + j * 8, 8), 8))
                elif p < 40:
                    v = q_ref[p - 8, rows, :]
                else:
                    v = above(pl.ds(pl.multiple_of((p - 40) * 64 + j * 8, 8), 8))
                for t in range(17):
                    i = p - t
                    if first <= i < first + 16:
                        term = v * taps0[t]
                        acc[i] = acc[i] + term if i in acc else term
            for i, value in acc.items():
                y0_ref[i, rows, :] = value
        return 0

    lax.fori_loop(0, 8, level0, 0)
    for i in range(32):
        store_pair(even_y, fa_ref, fb_ref, pl.ds(i * 8, 8), y0_ref[i, pl.ds(56, 8), :], y0_ref[i, pl.ds(0, 8), :])

    def received(ref, at, rows):
        if not 0 <= at < (11 if rows == 40 else 13):
            return None
        if at < 11:
            return ref(pl.ds(512 + at * 40, rows))
        return jnp.concatenate([ref(pl.ds(512 + ((at - 11) * 3 + k) * 40 + 24, 8)) for k in range(3)], axis=0)

    def added(values):
        values = [v for v in values if v is not None]
        total = values[0]
        for v in values[1:]:
            total = total + v
        return total

    def own(at, rows):
        if rows == 24 or at < 11:
            return received(sent_down, at, rows)
        return received(sent_up, at - 8, rows)

    for r in range(35):
        cell = r - 9
        q1[r] = added([own(cell + 1, 40), received(below, cell + 9, 40), received(above, cell - 15, 40)])
    for r in range(29):
        cell = r - 10
        q2[r] = added([own(cell + 2, 24), received(below, cell + 10, 24), received(above, cell - 6, 24)])
    start = jnp.where(ix < 2, 24, 0)
    mask = lanes_mask(OZ[2], EZ[2])
    for k, members in enumerate(FAR):
        for n, s in enumerate(members):
            q2[start + s] += jnp.where(mask, pltpu.roll(f_ref[k], (OZ[2] - n * EZ[2]) % 128, 1), 0.0)
    low = lanes_mask(0, EZ[1])
    two = {}

    def keep2(i, total):
        two[i] = masked(total, x_mask(2, LOW[2] + i))

    def keep1(s, total):
        total = masked(total, x_mask(1, LOW[1] + s))
        f, b = total[24:40], total[:16]
        o_ref[s, pl.ds(24, 16), :] = f
        o_ref[s, pl.ds(0, 24), :] = jnp.where(low, total[:24], two[s]) if s < EX[2] else total[:24]
        if s < EX[2]:
            f = jnp.where(low, f, two[s][8:])
            b = jnp.where(low, b, two[s][:16])
        store_pair(even_y, fa_ref, fb_ref, pl.ds(256 + s * 16, 16), f, b)

    for level in (3, 4):
        for t in range(17):
            tb_ref[pl.ds((level - 3) * 24 + t, 1), :] = jnp.full((1, 128), taps_ref[level, 0, t], F32)
    conv_x(EX[2], taps_ref, 2, lambda r: q2[r], keep2)
    conv_x(EX[1], taps_ref, 1, lambda r: q1[r], keep1)


def coarse_y_kernel(taps_ref, v_ref, u_ref):
    iy = lax.axis_index("gy")
    block = stacked(jnp.concatenate([v_ref[k] for k in range(8)], axis=0), 0, 1, 0)
    for level, first, last in ((3, 0, 256), (4, 256, 384)):
        i, j = iota((16, 384), 0), iota((16, 384), 1) & 127
        to = out_cells(level, BY, EY, i, iy, 8)
        d, r = j >> 4, j & 15
        at = jnp.where(r < EY[level], (d - iy) * BY[level] + r + LOW[level], BAD)
        out = dot(thirds(toeplitz(taps_ref, level, 1, at - to + 8), 128), block[:, first:last])
        for c in range(first, last, 128):
            u_ref[pl.ds(c // 8, 16), :] = out[:, c - first : c - first + 128]


def coarse_kernel(taps_ref, own_ref, r1_ref, r2_ref, r3_ref, z3_ref, z4_ref, t4_ref, g3, g4):
    ix = lax.axis_index("gx")
    for g in (g3, g4):
        g[...] = jnp.zeros_like(g)
    for ref, step in ((own_ref, 0), (r1_ref, 1), (r2_ref, 2), (r3_ref, 3)):
        source = ix ^ step
        for c, (level, members) in enumerate(V_COLUMNS):
            g = g3 if level == 3 else g4
            column = ref[pl.ds(c * 16, 16), :]
            for n, s in enumerate(members):
                g[source * BX[level] + (LOW[level] + s + 10)] += pltpu.roll(column, (OZ[level] - n * EZ[level]) % 128, 1)
    for level, g, z_ref in ((3, g3, z3_ref), (4, g4, z4_ref)):
        start = ix * BX[level] + 10 + LOW[level] - 8

        def keep(i, total, level=level, z_ref=z_ref):
            z_ref[pl.ds(i * 16, 16), :] = masked(total, x_mask(level, LOW[level] + i))

        conv_x(EX[level], taps_ref, level, lambda r, g=g, start=start: g[start + r], keep)
    t4_ref[...] = level4_rows(z4_ref)


BAD = 1000


def out_cells(level, blocks, ext, index, position, count):
    return jnp.where(in_grid(level, ext, blocks, count, index, position), index + LOW[level], -BAD)


def thirds(value, third):
    hi, lo = split(value)
    return jnp.where(iota(value.shape, 1) < 2 * third, hi.astype(F32), lo.astype(F32)).astype(BF16)


def toeplitz(taps_ref, level, axis, diff):
    total = jnp.zeros(diff.shape, F32)
    for t in range(17):
        total = jnp.where(diff == t, taps_ref[level, axis, t], total)
    return total


def store_z(ref, halo_ref, own, halo):
    ref[...] = jnp.concatenate(split(own), axis=1)
    hi, lo = split(halo)
    halo_ref[...] = jnp.concatenate([hi, hi, lo], axis=0)


def prep_y_kernel(taps_ref, *outs):
    iy = lax.axis_index("gy")
    for level, width, ref in ((0, 80, outs[0]), (1, 80, outs[1]), (2, 64, outs[2])):
        shape = (PY[level], 3 * width)
        i, j = iota(shape, 0), repeated(iota(shape, 1), width)
        to = out_cells(level, BY, EY, i, iy, 8)
        if level == 0:
            at = j - 8
        else:
            halo, reach = 16, 11 if level == 1 else 13
            own = j - halo
            upper = own - PY[level]
            lowest = LOW[level] - 8
            at = jnp.where(
                own < 0,
                jnp.where(j < reach, j + lowest, BAD),
                jnp.where(
                    upper < 0,
                    jnp.where(own < EY[level], own + LOW[level], BAD),
                    jnp.where(upper < reach, upper + LOW[level] + BY[level], BAD),
                ),
            )
        ref[...] = thirds(toeplitz(taps_ref, level, 1, at - to + 8), width)


def prep_z_kernel(taps_ref, *out):
    iy = lax.axis_index("gy")
    iz = lax.axis_index("gz")
    z_outs = [out[2 * k : 2 * k + 2] for k in range(5)]
    j = iota((128, 128), 0)
    c = iota((128, 128), 1)
    own = toeplitz(taps_ref, 0, 2, j - c + 8)
    j, c = iota((16, 128), 0), iota((16, 128), 1)
    store_z(*z_outs[0], own, toeplitz(taps_ref, 0, 2, jnp.where(j < 8, j - 8, j - 8 + 128) - c + 8))
    for level in range(4):
        out[10 + level][...] = prolong_y(level, iy)
    prolong = None
    for level in range(1, 5):
        shape = (128, 128)
        one = cubic_matrix(level - 1, EZ, BZ, 8, iz, iota(shape, 1), iota(shape, 0)).astype(BF16)
        whole = one.astype(F32) if prolong is None else dot(one, prolong[0]) + dot(one, prolong[1])
        prolong = split(whole)
        c = iota((128, 128), 1)
        to = out_cells(level, BZ, EZ, c, iz, 8)
        j = iota((128, 128), 0) - OZ[level]
        at = jnp.where((j >= 0) & (j < EZ[level]), j + LOW[level], BAD)
        own = dot3(split(toeplitz(taps_ref, level, 2, at - to + 8)), prolong)
        rows = 64 if level == 4 else 32
        c = iota((rows, 128), 1)
        to = out_cells(level, BZ, EZ, c, iz, 8)
        j = iota((rows, 128), 0)
        r = j & 15
        if level == 4:
            d = j >> 4
            shift = jnp.where(d == 0, -2, jnp.where(d == 1, -1, jnp.where(d == 2, 1, 2))) * BZ[4]
            at = jnp.where(r < EZ[4], shift + r + LOW[4], BAD)
        else:
            reach = 11 if level == 1 else 13
            at = jnp.where(j < 16, r + LOW[level] - 8, r + LOW[level] + BZ[level])
            at = jnp.where(r < reach, at, BAD)
        store_z(*z_outs[level], own, dot3(split(toeplitz(taps_ref, level, 2, at - to + 8)), prolong))


def level4_rows(z4_ref):
    block = pltpu.roll(z4_ref[...], (-OZ[4]) % 128, 1)
    return jnp.concatenate([block, jnp.zeros((16, 128), F32)], axis=0).T[:16]


def store_rows(even, a_ref, b_ref, at, up, down):
    store_pair(even, a_ref, b_ref, (slice(None), pl.ds(2048 + at, 128)), up[:8], down[:8])
    store_pair(even, a_ref, b_ref, (slice(None), pl.ds(3584 + at, 128)), up[8:], down[8:])


def load_rows(pick, at, count):
    return jnp.concatenate([pick((slice(None), pl.ds(2048 + at, count))), pick((slice(None), pl.ds(3584 + at, count)))], axis=0)


def y_kernel(y0_ref, o_ref, ra_ref, rb_ref, z3_ref, z4_ref, *refs):
    even, even_z = is_even("gy"), is_even("gz")
    below, above = picked(even, rb_ref, ra_ref), picked(even, ra_ref, rb_ref)
    my = [ref[...] for ref in refs[:3]]
    z0_ref, z1_ref, z2_ref, fa_ref, fb_ref = refs[3:]
    for base in range(0, 32, 4):
        parts = []
        for i in range(base, base + 4):
            parts.append(jnp.concatenate(
                [below(pl.ds(i * 8, 8)), y0_ref[i], above(pl.ds(i * 8, 8))], axis=0))
        out = dot(my[0], stacked(jnp.concatenate(parts, axis=1), 0, 1, 0))
        for n in range(4):
            z0_ref[pl.ds((base + n) * 64, 64), :] = out[:, n * 128 : (n + 1) * 128]
    for level, z_ref in ((1, z1_ref), (2, z2_ref)):
        n, rows = EX[level], PY[level]
        parts = [jnp.concatenate([below(pl.ds(256 + s * 16, 16)), o_ref[s, pl.ds(0, rows), :], above(pl.ds(256 + s * 16, 16))], axis=0)
                 for s in range(n)]
        out = dot(my[level], stacked(jnp.concatenate(parts, axis=1), 0, 1, 0))
        for s in range(n):
            z_ref[pl.ds(s * rows, rows), :] = out[:, s * 128 : (s + 1) * 128]
    for k in range(16):
        t = z0_ref[pl.ds(k * 128, 128), :].T
        store_pair(even_z, fa_ref, fb_ref, (slice(None), pl.ds(k * 128, 128)), t[120:], t[:8])
    for k in range(6):
        size = 128 if k < 5 else 120
        block = z1_ref[pl.ds(k * 128, size), :]
        if size < 128:
            block = jnp.concatenate([block, jnp.zeros((128 - size, 128), F32)], axis=0)
        t = block.T
        store_rows(even_z, fa_ref, fb_ref, k * 128, t[56:72], t[0:16])
    for level, z_ref, at, f, count in ((2, z2_ref, 768, 24, 312), (3, z3_ref, 1152, 8, 144)):
        for k in range((count + 127) // 128):
            size = min(128, count - k * 128)
            block = pltpu.roll(z_ref[pl.ds(k * 128, size), :], (-OZ[level]) % 128, 1)
            if size < 128:
                block = jnp.concatenate([block, jnp.zeros((128 - size, 128), F32)], axis=0)
            t = block.T
            store_rows(even_z, fa_ref, fb_ref, at + k * 128, t[f : f + 16], t[0:16])
    t = level4_rows(z4_ref)
    store_rows(even_z, fa_ref, fb_ref, 1408, t, t)


Z_AT = {0: 0, 1: 0, 2: 768, 3: 1152, 4: 1408}
Z_ROWS = {0: 2048, 1: 760, 2: 312, 3: 144, 4: 112}


def own_kernel(*refs):
    for level in range(5):
        z_ref, m_ref, t_ref = refs[level], refs[5 + level], refs[10 + level]
        m = m_ref[...]
        m = jnp.concatenate([m, jnp.concatenate([m[:, :128], jnp.zeros((128, 128), BF16)], axis=1)], axis=0)
        step = 512 if level == 0 else Z_ROWS[level]
        for k in range(0, Z_ROWS[level], step):
            both = dot(jnp.concatenate(split(z_ref[pl.ds(k, step), :]), axis=1), m)
            t_ref[pl.ds(k, step), :] = both[:, :128] + both[:, 128:]


def z_kernel(*refs):
    t_refs, (ra_ref, rb_ref, a4_ref, b4_ref), m_refs, py = refs[:5], refs[5:9], refs[9:14], refs[14:18]
    even, even2 = is_even("gz"), (lax.axis_index("gz") & 2) == 0
    below, above = picked(even, rb_ref, ra_ref), picked(even, ra_ref, rb_ref)
    below2, above2 = picked(even2, b4_ref, a4_ref), picked(even2, a4_ref, b4_ref)
    out_ref, acc = refs[18:]
    first = (((0,), (0,)), ((), ()))

    def halo_part(level, halo):
        return dot(stacked(halo, 0, 1, 0), m_refs[level][...], first)

    total = None
    for level in (4, 3, 2, 1):
        n = Z_ROWS[level]
        halo = [load_rows(ref, Z_AT[level], (n + 127) // 128 * 128) for ref in (below, above)]
        if level == 4:
            halo = [below2(...), *halo, above2(...)]
        term = t_refs[level][...] + halo_part(level, jnp.concatenate(halo, axis=0))[:n]
        planes = [term[s * PY[level] : (s + 1) * PY[level]] for s in range(EX[level])]
        if total is not None:
            planes = [a + b for a, b in zip(planes, total)]
        fine = level - 1
        wide = dot_left_exact(py[fine][...], jnp.concatenate(planes, axis=1))
        coarse = [wide[:, s * 128 : (s + 1) * 128] for s in range(EX[level])]
        total = []
        for cell in range(LOW[fine], LOW[fine] + EX[fine]):
            value = None
            for k, w in TAPS_AT:
                if (cell - k) % 2 == 0:
                    s = (cell - k) // 2 - LOW[level]
                    if 0 <= s < EX[level]:
                        part = coarse[s] if w == 1.0 else coarse[s] * w
                        value = part if value is None else value + part
            value = masked(value, x_mask(fine, cell)) if fine else value
            total.append(value)
            if fine == 0:
                acc[cell] = value
    halo = jnp.concatenate([pick((slice(None), pl.ds(0, 2048))) for pick in (below, above)], axis=0)
    for k in range(4):
        term = halo_part(0, halo[:, k * 512 : (k + 1) * 512])
        for i in range(8):
            s = k * 8 + i
            out_ref[s] = acc[s] + (t_refs[0][pl.ds(s * 64, 64), :] + term[i * 64 : (i + 1) * 64])


VMEM_LIMIT = 24 * 2**20
VM = pl.BlockSpec(memory_space=pltpu.VMEM)
SM = pl.BlockSpec(memory_space=pltpu.SMEM)


def call(body, shapes, in_specs, scratch=(), flops=4 * 10**8):
    return pl.pallas_call(
        body,
        out_shape=[jax.ShapeDtypeStruct(s, d) for s, d in shapes],
        in_specs=in_specs,
        out_specs=[VM] * len(shapes),
        scratch_shapes=list(scratch),
        compiler_params=pltpu.CompilerParams(vmem_limit_bytes=VMEM_LIMIT),
        cost_estimate=pl.CostEstimate(flops=flops, bytes_accessed=2**21, transcendentals=0),
    )


def prepared(body, shapes, taps):
    return call(body, [(w, BF16) for w in shapes], [SM])(taps)


def per_device(charges, kernel_taps):
    taps = kernel_taps

    def swap(v, axis, by=1, second=False):
        count = lax.axis_size(axis)
        partner = lambda i: i ^ by if not second else ((i + by) ^ by) - by
        return lax.ppermute(v, axis, [(i, partner(i)) for i in range(count) if 0 <= partner(i) < count])

    sa, sb, s2, v = call(
        restrict_kernel,
        [((952, 128), F32), ((952, 128), F32), ((2, 24, 128), F32),
         ((8, 16, 384), F32)],
        [VM], [pltpu.VMEM((13, 24, 128), F32)],
    )(charges)
    ra = swap(sa, "gx")
    rb = swap(sb, "gx", second=True)
    f2 = lax.ppermute(s2, "gx", [(i, i ^ 2) for i in range(4)])
    vs = lax.all_to_all(v, "gy", 0, 0)
    (u,) = call(coarse_y_kernel, [((48, 128), F32)], [SM, VM])(taps, vs)
    others = []
    for by in (1, 2, 3):
        others.append(lax.ppermute(u, "gx", [(i, i ^ by) for i in range(4)]))
    my = prepared(prep_y_kernel, [(64, 240), (40, 240), (24, 192)], taps)
    z_shapes = []
    for halo in (16, 32, 32, 32, 64):
        z_shapes += [(128, 256), (3 * halo, 128)]
    z_shapes += [(PY[l], 2 * up16(PY[l + 1])) for l in range(4)]
    mats = prepared(prep_z_kernel, z_shapes, taps)
    own, halo, py = mats[:10:2], mats[1:10:2], mats[10:]
    y0, o, sa, sb, tb = call(
        x_kernel,
        [((32, 64, 128), F32), ((19, 40, 128), F32), ((560, 128), F32), ((560, 128), F32), ((48, 128), F32)],
        [SM] + [VM] * 6,
        [pltpu.VMEM((35, 40, 128), F32), pltpu.VMEM((29, 24, 128), F32)],
    )(taps, charges, sa, sb, ra, rb, f2)
    ra = swap(sa, "gy")
    rb = swap(sb, "gy", second=True)
    z3, z4, t4 = call(
        coarse_kernel, [((144, 128), F32), ((112, 128), F32), ((16, 128), F32)], [VM] * 5,
        [pltpu.VMEM((37, 16, 128), F32), pltpu.VMEM((29, 16, 128), F32)],
    )(tb, u, *others)
    a4 = swap(t4, "gz", 2)
    b4 = swap(t4, "gz", 2, second=True)
    z0, z1, z2, sa, sb = call(
        y_kernel, [((Z_ROWS[l], 128), F32) for l in range(3)] + [((8, 5120), F32), ((8, 5120), F32)], [VM] * 9
    )(y0, o, ra, rb, z3, z4, *my)
    z = (z0, z1, z2, z3, z4)
    ra = swap(sa, "gz")
    rb = swap(sb, "gz", second=True)
    terms = call(own_kernel, [((Z_ROWS[l], 128), F32) for l in range(5)], [VM] * 10)(*z, *own)
    (out,) = call(
        z_kernel, [((32, 64, 128), F32)], [VM] * 18, [pltpu.VMEM((32, 64, 128), F32)]
    )(*terms, ra, rb, a4, b4, *halo, *py)
    return out


def solution(mesh):
    return jax.shard_map(
        per_device,
        mesh=mesh,
        in_specs=(P("gx", "gy", "gz"), P()),
        out_specs=P("gx", "gy", "gz"),
        check_vma=False,
    )
```
